128 devices in a mesh: expert: 64 (over y, x, z), etp: 2 (over core).
Axes of the slice: x: 4, y: 4, z: 4, core: 2. Of those that a mesh axis runs over, the one named last changes fastest.
Arguments:
- grad_out: bfloat16 [8192, 3584], P('expert', 'etp'), may hold values from -6 to 6
- combine: bfloat16 [8192, 8], P('expert'), may hold values from 0.099609375 to 2.5
- expert_ids: int32 [8192, 8], P('expert'), may hold values from 0 to 127, all different within a row; in each aligned block of 128 rows (0 to 127, 128 to 255, ...) at most 16 rows name the same one
- saved_gate: bfloat16 [1024, 128, 1024], P(None, 'expert', 'etp'), may hold values from -6 to 6
- saved_up: bfloat16 [1024, 128, 1024], P(None, 'expert', 'etp'), may hold values from -1.5 to 1.5
- gate_weight: bfloat16 [128, 3584, 1024], P('expert', None, 'etp'), may hold values from -0.09375 to 0.09375
- up_weight: bfloat16 [128, 3584, 1024], P('expert', None, 'etp'), may hold values from -0.09375 to 0.09375
- down_weight: bfloat16 [128, 1024, 3584], P('expert', 'etp'), may hold values from -0.09375 to 0.09375
Outputs:
- grad_tokens: bfloat16 [8192, 3584], P('expert', 'etp')
- grad_combine: bfloat16 [8192, 8], P('expert')
The draws below stay inside these ranges and needn't reach their ends.
Inputs may be any that keep to these rules, and one draw needn't show every extreme that they name: `expert_ids`: each token names 8 different experts. Among the 128 tokens of one block (one index of expert), at most 16 name any one expert, and some blocks reach that bound.
All inputs are finite; a program needn't handle non-finite values.
Results may differ from the reference program's by a relative error of at most 0.012.
Values may be sent and summed in bfloat16 or wider, within the bound.
A program may use at most 192 MiB of HBM per device.

```python
import math
import jax
import jax.numpy as jnp
import numpy as np
from jax import lax

D = 3584
FF = 1024
TOP = 8
TOK_DEV = 128
EXPERTS = 128
TOKENS = 8192
CAP = 16
SLOT_ROWS = 1024
N_EXPERT = 64
N_ETP = 2


def steps_of(stream_key, extent, shards, smallest, top_value):
    gain = 1.0
    for axis_at, parts in shards:
        draws = jax.random.uniform(jax.random.fold_in(jax.random.fold_in(stream_key, 6), axis_at), (parts,), jnp.float32, smallest / len(shards), top_value / len(shards))
        gain = gain * jnp.repeat(jnp.exp(draws), extent[axis_at] // parts).reshape((-1,) + (1,) * (len(extent) - 1 - axis_at))
    return gain


def shared_out(rng, own, number, rows, amount, top, limit, slope):
    sequence = jax.random.permutation(rng, amount)
    crowded, ordinary = portions_of(amount, rows * top, limit, slope, True), portions_of(amount, rows * top, limit, slope, False)
    places = jnp.arange(amount)

    def named(sizes, rotation):
        used = int((sizes > 0).sum())
        fixed = max(1, used // 4)
        passed = fixed + (places - fixed + rotation * (used - fixed)) % max(1, amount - fixed)
        return jnp.zeros((amount,), jnp.int32).at[sequence[jnp.where(places < fixed, places, passed)]].set(jnp.asarray(sizes, jnp.int32))

    sizes = jnp.where(number % 4 == 0, named(crowded, number // 4), named(ordinary, number - number // 4 - 1))
    mixed = jax.random.permutation(jax.random.fold_in(own, 3), amount)
    source_of, taker = mixed[0:amount // 2 * 2:2], mixed[1:amount // 2 * 2:2]
    room = jnp.minimum(sizes[source_of] - 1, limit - sizes[taker]) // 2
    room = jnp.where((source_of == sequence[0]) | (taker == sequence[0]) | (sizes[taker] == 0), 0, jnp.maximum(room, 0))
    passed = jax.random.randint(jax.random.fold_in(own, 4), (amount // 2,), 0, 1 << 20) % (room + 1)
    sizes = sizes.at[source_of].add(-passed).at[taker].add(passed)
    labels = jnp.searchsorted(jnp.cumsum(sizes), jnp.arange(rows * top), side="right").astype(jnp.int32)
    grid = labels.reshape(top, rows).T
    grid = grid[jax.random.permutation(jax.random.fold_in(own, 1), rows)]
    rotation = jax.random.randint(jax.random.fold_in(own, 2), (rows, 1), 0, top)
    return jnp.take_along_axis(grid, (jnp.arange(top)[None, :] + rotation) % top, axis=1)


def portions_of(count, total, bound, slope, full):
    loads = [(1 << 20) // math.isqrt(standing ** slope) + 1 for standing in range(1, count + 1)]
    largest = bound if full else min(bound, max(-(-total // count), total * loads[0] // sum(loads)))
    least = 1 if total - largest >= count - 1 else 0
    given, spare = [largest] + [least] * (count - 1), total - largest - least * (count - 1)
    while spare > 0:
        free = [i for i in range(1, count) if given[i] < largest] or [i for i in range(1, count) if given[i] < bound]
        whole, remaining = sum([loads[i] for i in free]), spare
        for i in free:
            more = min(bound - given[i], max(1, remaining * loads[i] // whole), spare)
            given[i] = given[i] + more
            spare = spare - more
    return np.array(given)


def gaussian(key, extent, spread, most, cuts=(), held_as=jnp.bfloat16):
    level = steps_of(key, extent, cuts, -0.22, 0.18) if cuts else 1.0
    drawn = jax.random.normal(key, extent, jnp.float32) * spread * level
    return jnp.minimum(jnp.maximum(drawn, -most), most).astype(held_as)


def setup_inputs(seed: int = 0) -> dict:
    keys = jax.random.split(jax.random.key(seed), 9)
    grad_out = gaussian(keys[0], (TOKENS, D), 1.0, 6.0, ((0, 64), (1, 2)))
    combine = jnp.clip(jnp.exp(math.log(2.5) - 3.2227897 * jax.random.uniform(keys[1], (TOKENS, TOP), jnp.float32) ** steps_of(keys[1], (TOKENS, TOP), ((0, 64),), -0.2, 0.2)), 0.099609375, 2.5).astype(jnp.bfloat16)
    expert_ids_keys = jax.random.split(jax.random.fold_in(keys[2], 1), TOKENS // TOK_DEV)
    expert_ids_turns = jax.random.permutation(jax.random.fold_in(keys[2], 3), TOKENS // TOK_DEV)
    expert_ids = jax.vmap(lambda own, number: shared_out(jax.random.fold_in(keys[2], 2), own, number, TOK_DEV, EXPERTS, TOP, CAP, 2))(expert_ids_keys, expert_ids_turns).reshape((TOKENS, TOP))
    saved_gate = gaussian(keys[3], (SLOT_ROWS, EXPERTS, FF), 1.0, 6.0, ((1, 64), (2, 2)))
    saved_up = gaussian(keys[4], (SLOT_ROWS, EXPERTS, FF), 0.1, 1.5, ((1, 64), (2, 2)))
    gate_weight = gaussian(keys[5], (EXPERTS, D, FF), D ** -0.5, 0.09375, ((0, 64), (2, 2)))
    up_weight = gaussian(keys[6], (EXPERTS, D, FF), D ** -0.5, 0.09375, ((0, 64), (2, 2)))
    down_weight = gaussian(keys[7], (EXPERTS, FF, D), D ** -0.5, 0.09375, ((0, 64), (1, 2)))
    return dict(grad_out=grad_out, combine=combine, expert_ids=expert_ids, saved_gate=saved_gate, saved_up=saved_up, gate_weight=gate_weight, up_weight=up_weight, down_weight=down_weight)


def reference(grad_out, combine, expert_ids, saved_gate, saved_up, gate_weight, up_weight, down_weight):
    token_total, top_count = expert_ids.shape
    experts, model_width, hidden = gate_weight.shape
    groups = N_EXPERT
    token_count = token_total // groups
    capacity = saved_gate.shape[0] // groups
    slot_total = groups * capacity
    grouped = expert_ids.reshape(groups, token_count, top_count)
    matches = grouped[..., None] == jnp.arange(experts, dtype=jnp.int32)
    expert_loads = jnp.sum(matches.astype(jnp.int32), axis=2)
    earlier = jnp.cumsum(expert_loads, axis=1) - expert_loads
    position = jnp.sum(jnp.where(matches, earlier[:, :, None, :], 0), axis=3)
    row_index = (jnp.arange(groups, dtype=jnp.int32)[:, None, None] * capacity + position).reshape(token_total, top_count)
    slot_owner = jnp.full((slot_total, experts), token_total * top_count, jnp.int32)
    slot_owner = slot_owner.at[row_index.reshape(-1), expert_ids.reshape(-1)].set(
        jnp.arange(token_total * top_count, dtype=jnp.int32))
    grad_padded = jnp.concatenate([grad_out, jnp.zeros((1, model_width), jnp.bfloat16)], axis=0)
    weight_padded = jnp.concatenate([combine.reshape(-1).astype(jnp.float32), jnp.zeros((1,), jnp.float32)])
    half_hidden = hidden // N_ETP

    def per_expert(running, expert):
        grad_acc, weight_acc = running
        slot_ids = lax.dynamic_index_in_dim(slot_owner, expert, 1, keepdims=False)
        token_of = slot_ids // top_count
        slot_rows = jnp.take(grad_padded, token_of, axis=0)
        slot_weight = jnp.take(weight_padded, slot_ids, axis=0)
        gate_value = lax.dynamic_index_in_dim(saved_gate, expert, 1, keepdims=False).astype(jnp.float32)
        up_value = lax.dynamic_index_in_dim(saved_up, expert, 1, keepdims=False).astype(jnp.float32)
        down_expert = lax.dynamic_index_in_dim(down_weight, expert, 0, keepdims=False)
        gate_expert = lax.dynamic_index_in_dim(gate_weight, expert, 0, keepdims=False)
        up_expert = lax.dynamic_index_in_dim(up_weight, expert, 0, keepdims=False)
        grad_hidden = jnp.dot(slot_rows, down_expert.T, preferred_element_type=jnp.float32)
        gate_sigmoid = jax.nn.sigmoid(gate_value)
        activated = gate_value * gate_sigmoid
        product = grad_hidden * activated * up_value
        weight_halves = jnp.sum(product.reshape(slot_total, N_ETP, half_hidden), axis=2).astype(jnp.bfloat16)
        weight_halves = lax.optimization_barrier(weight_halves).astype(jnp.float32)
        slot_dw = jnp.sum(weight_halves, axis=1).astype(jnp.bfloat16)
        scaled = slot_weight[:, None] * grad_hidden
        grad_gate = (scaled * up_value * gate_sigmoid * (1.0 + gate_value * (1.0 - gate_sigmoid))).astype(jnp.bfloat16)
        grad_up = (scaled * activated).astype(jnp.bfloat16)
        running_sum = jnp.zeros((slot_total, model_width), jnp.float32)
        for half_index in range(N_ETP):
            lower = half_index * half_hidden
            term_half = jnp.dot(grad_gate[:, lower:lower + half_hidden], gate_expert[:, lower:lower + half_hidden].T,
                                preferred_element_type=jnp.float32)
            term_half = term_half + jnp.dot(grad_up[:, lower:lower + half_hidden], up_expert[:, lower:lower + half_hidden].T,
                                            preferred_element_type=jnp.float32)
            term_half = lax.optimization_barrier(term_half.astype(jnp.bfloat16))
            running_sum = running_sum + term_half.astype(jnp.float32)
        slot_grad = running_sum.astype(jnp.bfloat16)
        grad_acc = grad_acc.at[token_of].add(slot_grad.astype(jnp.float32), mode="drop")
        weight_acc = weight_acc.at[slot_ids].set(slot_dw.astype(jnp.float32), mode="drop")
        return (grad_acc, weight_acc), None

    start = (jnp.zeros((token_total, model_width), jnp.float32), jnp.zeros((token_total * top_count,), jnp.float32))
    final, _ = lax.scan(per_expert, start, jnp.arange(experts, dtype=jnp.int32))
    grad_tokens = final[0].astype(jnp.bfloat16)
    grad_combine = final[1].reshape(token_total, top_count).astype(jnp.bfloat16)
    return grad_tokens, grad_combine
```

```python
import functools
import itertools

import jax
import jax.numpy as jnp
from jax import lax
from jax.experimental import pallas as pl
from jax.experimental.pallas import tpu as pltpu
from jax.sharding import PartitionSpec as P

MESH = pl.DeviceIdType.MESH
BF16, F32, I32 = jnp.bfloat16, jnp.float32, jnp.int32
NT = (((1,), (1,)), ((), ()))
TN = (((0,), (0,)), ((), ()))
CAP = 16
AXES = ((0, 1, 2), (1, 2, 0), (2, 0, 1))


class Plan:
    def __init__(self, n, half, ff, top, tiles, step):
        self.n, self.half, self.ff, self.top, self.step = n, half, ff, top, step
        self.part = (half + 128) // 3
        self.wide = 3 * self.part
        self.widths = (self.part, self.part, self.part - 128)
        self.order = sorted(itertools.product(range(n), repeat=3), key=lambda d: (max(d), d))
        self.slot = {d: i for i, d in enumerate(self.order)}
        self.tiles, start = [], 0
        for count in tiles:
            self.tiles.append((start, count))
            start += count
        self.most = max(tiles)
        self.planes = n * n
        self.peers = [d for d in self.order if 0 < sum(v > 0 for v in d) < 3]

    def along(self, f, values):
        out = [0, 0, 0]
        for axis, value in zip(AXES[f], values):
            out[axis] = value
        return tuple(out)

    def seen(self, f, d):
        return tuple(d[axis] for axis in AXES[f])


def kernel(p, ids_ref, cw_ref, go_ref, sg_ref, su_ref, gw_ref, uw_ref, dn_ref, gt_ref, gc_ref,
           xo, xp, uin, s0, s1, s2, r0, r1, r2, g0, g1, g2, gm, ts, tr, gcs, gcr, codes, cws, meta,
           dno, dnp, gwo, gwp, uwo, uwp, sgt, sut, gbuf, ggb, gub,
           wsem, s1s, s1r, ds, dr, fs, fr, us, ur, rs, rr, tss, trs, sas, credit):
    n, half, part, planes = p.n, p.half, p.part, p.planes
    send, back, gath = (s0, s1, s2), (r0, r1, r2), (g0, g1, g2)
    me, core = lax.axis_index("expert"), lax.axis_index("etp")
    at = (me // (n * n), lax.rem(me // n, n), lax.rem(me, n))
    stride = (n * n, n, 1)

    def device(d, sign=1):
        c = [lax.rem(v + (sign * o) % n, n) for v, o in zip(at, d)]
        return (c[0] * stride[0] + c[1] * stride[1] + c[2], core)

    partner = (me, 1 - core)

    def block_of(d):
        return device(d, -1)[0]

    own = pl.multiple_of(core * half, 128)
    other = pl.multiple_of((1 - core) * half, 128)
    loads = [
        pltpu.make_async_copy(dn_ref.at[:, :, pl.ds(own, half)], dno, wsem.at[0]),
        pltpu.make_async_copy(dn_ref.at[:, :, pl.ds(other, half)], dnp, wsem.at[1]),
        pltpu.make_async_copy(gw_ref.at[:, pl.ds(other, half), :], gwp, wsem.at[2]),
        pltpu.make_async_copy(uw_ref.at[:, pl.ds(other, half), :], uwp, wsem.at[3]),
        pltpu.make_async_copy(gw_ref.at[:, pl.ds(own, half), :], gwo, wsem.at[4]),
        pltpu.make_async_copy(uw_ref.at[:, pl.ds(own, half), :], uwo, wsem.at[5]),
    ]
    for load in loads:
        load.start()

    def saved_start(t):
        first, count = p.tiles[t]
        for j in range(count):
            b = block_of(p.order[first + j])
            pltpu.make_async_copy(sg_ref.at[b], sgt.at[j], sas.at[0]).start()
            pltpu.make_async_copy(su_ref.at[b], sut.at[j], sas.at[1]).start()

    def saved_wait(t):
        count = p.tiles[t][1]
        pltpu.make_async_copy(sg_ref.at[pl.ds(0, count)], sgt.at[pl.ds(0, count)], sas.at[0]).wait()
        pltpu.make_async_copy(su_ref.at[pl.ds(0, count)], sut.at[pl.ds(0, count)], sas.at[1]).wait()

    saved_start(0)

    barrier = pltpu.get_barrier_semaphore()
    for d in p.peers:
        pl.semaphore_signal(barrier, inc=1, device_id=device(d), device_id_type=MESH)
    pl.semaphore_signal(barrier, inc=1, device_id=partner, device_id_type=MESH)

    meta[...] = jnp.concatenate(
        [ids_ref[...].astype(F32), cw_ref[...].astype(F32)], axis=0
    ).astype(BF16)
    tokens = meta.shape[1]
    before = (
        lax.broadcasted_iota(I32, (tokens, tokens), 0)
        < lax.broadcasted_iota(I32, (tokens, tokens), 1)
    ).astype(F32).astype(BF16)
    rows = 2 * planes
    r_iota = lax.broadcasted_iota(I32, (rows, tokens), 0)

    def experts_of(f):
        a, b, c = AXES[f]
        place = r_iota // 2
        vb = lax.rem(at[b] + place // n, n)
        vc = lax.rem(at[c] + lax.rem(place, n), n)
        return 2 * (at[a] * stride[a] + vb * stride[b] + vc * stride[c]) + lax.rem(r_iota, 2)

    experts = [experts_of(f).astype(F32) for f in range(3)]
    c_iota = lax.broadcasted_iota(I32, (rows, CAP, tokens), 1).astype(F32)

    def select(f, a, info, token_cols):
        info = info.astype(F32)
        match = jnp.zeros((rows, tokens), F32)
        weight = jnp.zeros((rows, tokens), F32)
        for k in range(p.top):
            hit = experts[f] == info[k:k + 1, :]
            match = jnp.where(hit, 1.0, match)
            weight = jnp.where(hit, info[p.top + k:p.top + k + 1, :], weight)
        position = jnp.dot(match.astype(BF16), before, preferred_element_type=F32)
        code = jnp.where(match > 0, position, -1.0)
        codes[f, a] = code
        cws[f, a] = weight
        hot = jnp.where(code[:, None, :] == c_iota, 1.0, 0.0)
        hot = hot.reshape(rows * CAP, tokens).astype(BF16)
        width = p.widths[f]
        own_slot = p.slot[p.along(f, (a, 0, 0))]
        for lo in range(0, width, 256):
            hi = min(lo + 256, width)
            picked = jnp.dot(hot, token_cols(lo, hi), preferred_element_type=F32).astype(BF16)
            picked = picked.reshape(planes, 2, CAP, hi - lo)
            send[f][a, :, :, :, lo:hi] = picked
            xo[own_slot, :, :, f * part + lo:f * part + hi] = picked[0]

    def dispatch_copy(f, a, q):
        b, c = q // n, q % n
        width = p.widths[f]
        slot = p.slot[p.along(f, (a, b, c))]
        return pltpu.make_async_remote_copy(
            src_ref=send[f].at[a, q],
            dst_ref=xo.at[slot, :, :, pl.ds(f * part, width)],
            send_sem=ds.at[f, a],
            recv_sem=dr.at[f, slot],
            device_id=device(p.along(f, (0, b, c))),
            device_id_type=MESH,
        )

    def gather_copies(f, o):
        to = device(p.along(f, (o, 0, 0)))
        return (
            pltpu.make_async_remote_copy(
                src_ref=go_ref.at[:, pl.ds(f * part, p.widths[f])],
                dst_ref=gath[f].at[o - 1],
                send_sem=s1s.at[f, o - 1, 0], recv_sem=s1r.at[f, o - 1, 0],
                device_id=to, device_id_type=MESH),
            pltpu.make_async_remote_copy(
                src_ref=meta, dst_ref=gm.at[f, o - 1],
                send_sem=s1s.at[f, o - 1, 1], recv_sem=s1r.at[f, o - 1, 1],
                device_id=to, device_id_type=MESH),
        )

    pl.semaphore_wait(barrier, len(p.peers) + 1)
    for o in range(1, n):
        for f in range(3):
            for copy in gather_copies(f, o):
                copy.start()
    for f in range(3):
        select(f, 0, meta[...], lambda lo, hi: go_ref[:, f * part + lo:f * part + hi])
        for q in range(1, planes):
            dispatch_copy(f, 0, q).start()
    for a in range(1, n):
        for f in range(3):
            for copy in gather_copies(f, a):
                copy.wait_recv()
            select(f, a, gm[f, a - 1], lambda lo, hi: gath[f][a - 1, :, lo:hi])
            for q in range(1, planes):
                dispatch_copy(f, a, q).start()

    def forward_copy(t, lo, count):
        return pltpu.make_async_remote_copy(
            src_ref=xo.at[pl.ds(lo, count), :, :, pl.ds(0, half)],
            dst_ref=xp.at[pl.ds(lo, count), :, :, pl.ds(0, half)],
            send_sem=fs.at[t], recv_sem=fr.at[t],
            device_id=partner, device_id_type=MESH)

    def return_copy(f, t, slot):
        a, b, c = p.seen(f, p.order[slot])
        return pltpu.make_async_remote_copy(
            src_ref=xo.at[slot, :, :, pl.ds(f * part, part)],
            dst_ref=back[f].at[a, b * n + c],
            send_sem=rs.at[f, t], recv_sem=rr.at[f, a],
            device_id=device(p.along(f, (0, b, c)), -1), device_id_type=MESH)

    for t, (first, count) in enumerate(p.tiles):
        m = count * CAP
        for slot in range(first, first + count):
            for f in range(3):
                a, b, c = p.seen(f, p.order[slot])
                if (b, c) != (0, 0):
                    dispatch_copy(f, a, b * n + c).wait_recv()
            forward_copy(t, slot, 1).start()
        saved_wait(t)
        if t == 0:
            loads[0].wait()
            loads[1].wait()
        forward_copy(t, first, count).wait_recv()
        if t == 0:
            for load in loads[2:]:
                load.wait()

        def hidden(l, _):
            x_own = xo[pl.ds(first, count), l, :, 0:half].reshape(m, half)
            x_oth = xp[pl.ds(first, count), l, :, 0:half].reshape(m, half)
            g = lax.dot_general(x_own, dno[l], NT, preferred_element_type=F32)
            g = g + lax.dot_general(x_oth, dnp[l], NT, preferred_element_type=F32)
            gbuf[0:m, :] = g

            def pointwise(j, _):
                at_row = pl.ds(pl.multiple_of(j * CAP, CAP), CAP)
                grad = gbuf[at_row, :]
                gate = sgt[j, l].astype(F32)
                up = sut[j, l].astype(F32)
                sig = 0.5 * jnp.tanh(0.5 * gate) + 0.5
                act = gate * sig
                gup = grad * act
                total = jnp.sum(gup * up, axis=1, keepdims=True)
                xp[first + j, l, :, half:half + 128] = jnp.broadcast_to(total, (CAP, 128)).astype(BF16)
                ggb[l, at_row, :] = (grad * up * sig * (1.0 + gate * (1.0 - sig))).astype(BF16)
                gub[l, at_row, :] = gup.astype(BF16)
                return 0

            lax.fori_loop(0, count, pointwise, 0)
            project(l, gwp, uwp, xp)
            return 0

        def project(l, gate_w, up_w, into):
            gg, gu = ggb[l, 0:m, :], gub[l, 0:m, :]
            for lo in range(0, half, p.step):
                u = lax.dot_general(gg, gate_w[l, lo:lo + p.step, :], NT, preferred_element_type=F32)
                u = u + lax.dot_general(gu, up_w[l, lo:lo + p.step, :], NT, preferred_element_type=F32)
                into[pl.ds(first, count), l, :, lo:lo + p.step] = u.astype(BF16).reshape(count, CAP, p.step)

        lax.fori_loop(0, 2, hidden, 0)
        if t + 1 < len(p.tiles):
            saved_start(t + 1)
        if t > 0:
            pl.semaphore_wait(credit, 1)
        swap = pltpu.make_async_remote_copy(
            src_ref=xp.at[pl.ds(first, count)], dst_ref=uin.at[pl.ds(0, count)],
            send_sem=us.at[t], recv_sem=ur.at[t], device_id=partner, device_id_type=MESH)
        swap.start()
        forward_copy(t, first, count).wait_send()

        def keep(l, _):
            project(l, gwo, uwo, xo)
            xo[pl.ds(first, count), l, :, half:half + 128] = xp[pl.ds(first, count), l, :, half:half + 128]
            return 0

        lax.fori_loop(0, 2, keep, 0)
        swap.wait_recv()

        def add(j, _):
            xo[first + j] = (xo[first + j].astype(F32) + uin[j].astype(F32)).astype(BF16)
            return 0

        lax.fori_loop(0, count, add, 0)
        if t + 1 < len(p.tiles):
            pl.semaphore_signal(credit, inc=1, device_id=partner, device_id_type=MESH)
        for slot in range(first, first + count):
            for f in range(3):
                a, b, c = p.seen(f, p.order[slot])
                if (b, c) == (0, 0):
                    back[f][a, 0] = xo[slot, :, :, f * part:(f + 1) * part]
                else:
                    return_copy(f, t, slot).start()

    def total_copy(f, o):
        to = device(p.along(f, (o, 0, 0)), -1)
        width = p.widths[f]
        copies = [pltpu.make_async_remote_copy(
            src_ref=ts.at[f, o - 1, :, pl.ds(0, width)], dst_ref=tr.at[f, o - 1, :, pl.ds(0, width)],
            send_sem=tss.at[f, o - 1, 0], recv_sem=trs.at[f, o - 1, 0],
            device_id=to, device_id_type=MESH)]
        if f == 2:
            copies.append(pltpu.make_async_remote_copy(
                src_ref=gcs.at[o - 1], dst_ref=gcr.at[o - 1],
                send_sem=tss.at[f, o - 1, 1], recv_sem=trs.at[f, o - 1, 1],
                device_id=to, device_id_type=MESH))
        return copies

    def back_wait(f, a):
        pltpu.make_async_remote_copy(
            src_ref=xo.at[pl.ds(0, planes - 1), :, :, pl.ds(0, part)],
            dst_ref=back[f].at[a, pl.ds(1, planes - 1)],
            send_sem=rs.at[f, 0], recv_sem=rr.at[f, a],
            device_id=partner, device_id_type=MESH).wait_recv()

    def combined(f, a, info):
        back_wait(f, a)
        hit = codes[f, a][:, None, :] == c_iota
        weight = jnp.where(hit, cws[f, a][:, None, :], 0.0)
        weight = weight.reshape(rows * CAP, tokens).astype(BF16)
        width = p.widths[f]
        values = back[f][a, :, :, :, 0:width].reshape(rows * CAP, width)
        total = lax.dot_general(weight, values, TN, preferred_element_type=F32)
        if f < 2:
            return total, None
        hot = jnp.where(hit, 1.0, 0.0).reshape(rows * CAP, tokens).astype(BF16)
        sums = back[f][a, :, :, :, width:part].reshape(rows * CAP, 128)
        lane = lax.broadcasted_iota(I32, (rows * CAP, 128), 1)
        row = lax.broadcasted_iota(I32, (rows * CAP, 128), 0) // CAP
        sums = jnp.where(lane == row, sums.astype(F32), 0.0).astype(BF16)
        spread = lax.dot_general(sums, hot, TN, preferred_element_type=F32)[0:rows]
        info = info.astype(F32)
        picked = [
            jnp.sum(jnp.where(experts[f] == info[k:k + 1, :], spread, 0.0), axis=0, keepdims=True)
            for k in range(p.top)
        ]
        return total, jnp.concatenate(picked, axis=0)

    for a in range(1, n):
        for f in range(3):
            total, sums = combined(f, a, gm[f, a - 1])
            ts[f, a - 1, :, 0:p.widths[f]] = total.astype(BF16)
            if f == 2:
                gcs[a - 1] = sums
            for copy in total_copy(f, a):
                copy.start()
    for f in range(3):
        total, sums = combined(f, 0, meta[...])
        width = p.widths[f]
        for a in range(1, n):
            for copy in total_copy(f, a):
                copy.wait_recv()
            total = total + tr[f, a - 1, :, 0:width].astype(F32)
            if f == 2:
                sums = sums + gcr[a - 1]
        gt_ref[:, f * part:f * part + width] = total.astype(BF16)
        if f == 2:
            gc_ref[...] = sums.astype(BF16)

    for f in range(3):
        width = p.widths[f]
        for o in range(1, n):
            for copy in gather_copies(f, o) + tuple(total_copy(f, o)):
                copy.wait_send()
        for a in range(n):
            pltpu.make_async_remote_copy(
                src_ref=send[f].at[a, pl.ds(1, planes - 1)],
                dst_ref=send[f].at[a, pl.ds(1, planes - 1)],
                send_sem=ds.at[f, a], recv_sem=dr.at[f, 0],
                device_id=partner, device_id_type=MESH).wait_send()
        for t, (first, count) in enumerate(p.tiles):
            sent = sum(p.seen(f, p.order[s])[1:] != (0, 0) for s in range(first, first + count))
            if sent:
                pltpu.make_async_remote_copy(
                    src_ref=xo.at[pl.ds(0, sent), :, :, pl.ds(0, part)],
                    dst_ref=xp.at[pl.ds(0, sent), :, :, pl.ds(0, part)],
                    send_sem=rs.at[f, t], recv_sem=rr.at[f, 0],
                    device_id=partner, device_id_type=MESH).wait_send()
    for t, (first, count) in enumerate(p.tiles):
        pltpu.make_async_remote_copy(
            src_ref=xp.at[pl.ds(first, count)], dst_ref=uin.at[pl.ds(0, count)],
            send_sem=us.at[t], recv_sem=ur.at[t], device_id=partner, device_id_type=MESH).wait_send()


def on_device(plan, grad_out, combine, expert_ids, saved_gate, saved_up, gate_weight, up_weight, down_weight):
    p = plan
    n, half, ff, part, planes = p.n, p.half, p.ff, p.part, p.planes
    tokens, top = expert_ids.shape
    blocks, nt = n * n * n, len(p.tiles)
    saved = [
        jnp.transpose(v.reshape(blocks, CAP, 2, ff), (0, 2, 1, 3)) for v in (saved_gate, saved_up)
    ]
    vmem = pl.BlockSpec(memory_space=pltpu.VMEM)
    hbm = pl.BlockSpec(memory_space=pl.ANY)
    dma, regular = pltpu.SemaphoreType.DMA, pltpu.SemaphoreType.REGULAR
    rows = 2 * planes
    scratch = [
        pltpu.VMEM((blocks, 2, CAP, p.wide), BF16),
        pltpu.VMEM((blocks, 2, CAP, p.wide), BF16),
        pltpu.VMEM((p.most, 2, CAP, p.wide), BF16),
        *[pltpu.VMEM((n, planes, 2, CAP, w), BF16) for w in p.widths],
        *[pltpu.VMEM((n, planes, 2, CAP, part), BF16) for _ in range(3)],
        *[pltpu.VMEM((n - 1, tokens, w), BF16) for w in p.widths],
        pltpu.VMEM((3, n - 1, 2 * top, tokens), BF16),
        pltpu.VMEM((3, n - 1, tokens, part), BF16),
        pltpu.VMEM((3, n - 1, tokens, part), BF16),
        pltpu.VMEM((n - 1, top, tokens), F32),
        pltpu.VMEM((n - 1, top, tokens), F32),
        pltpu.VMEM((3, n, rows, tokens), F32),
        pltpu.VMEM((3, n, rows, tokens), F32),
        pltpu.VMEM((2 * top, tokens), BF16),
        pltpu.VMEM((2, ff, half), BF16),
        pltpu.VMEM((2, ff, half), BF16),
        *[pltpu.VMEM((2, half, ff), BF16) for _ in range(4)],
        pltpu.VMEM((p.most, 2, CAP, ff), BF16),
        pltpu.VMEM((p.most, 2, CAP, ff), BF16),
        pltpu.VMEM((p.most * CAP, ff), F32),
        pltpu.VMEM((2, p.most * CAP, ff), BF16),
        pltpu.VMEM((2, p.most * CAP, ff), BF16),
        dma((6,)), dma((3, n - 1, 2)), dma((3, n - 1, 2)), dma((3, n)), dma((3, blocks)),
        dma((nt,)), dma((nt,)), dma((nt,)), dma((nt,)), dma((3, nt)), dma((3, n)),
        dma((3, n - 1, 2)), dma((3, n - 1, 2)), dma((2,)), regular,
    ]
    grad_tokens, grad_combine = pl.pallas_call(
        functools.partial(kernel, p),
        out_shape=(
            jax.ShapeDtypeStruct((tokens, half), BF16),
            jax.ShapeDtypeStruct((top, tokens), BF16),
        ),
        in_specs=[vmem, vmem, vmem, hbm, hbm, hbm, hbm, hbm],
        out_specs=(vmem, vmem),
        scratch_shapes=scratch,
        compiler_params=pltpu.CompilerParams(
            collective_id=0, has_side_effects=True, vmem_limit_bytes=67043328
        ),
    )(expert_ids.T, combine.T, grad_out, *saved, gate_weight, up_weight, down_weight)
    return grad_tokens, grad_combine.T


def solution(mesh, tiles=(8, 19, 19, 18), step=256):
    n = round(mesh.shape["expert"] ** (1 / 3))

    def run(grad_out, combine, expert_ids, saved_gate, saved_up, gate_weight, up_weight, down_weight):
        plan = Plan(n, grad_out.shape[1], gate_weight.shape[2], expert_ids.shape[1], tiles, step)
        return on_device(
            plan, grad_out, combine, expert_ids, saved_gate, saved_up, gate_weight, up_weight, down_weight
        )

    in_specs = (
        P("expert", "etp"),
        P("expert", None),
        P("expert", None),
        P(None, "expert", "etp"),
        P(None, "expert", "etp"),
        P("expert", None, "etp"),
        P("expert", None, "etp"),
        P("expert", "etp", None),
    )
    out_specs = (P("expert", "etp"), P("expert", None))
    return jax.shard_map(run, mesh=mesh, in_specs=in_specs, out_specs=out_specs, check_vma=False)
```

```python
import functools
import itertools

import jax
import jax.numpy as jnp
from jax import lax
from jax.experimental import pallas as pl
from jax.experimental.pallas import tpu as pltpu
from jax.sharding import PartitionSpec as P

MESH = pl.DeviceIdType.MESH
BF16, F32, I32 = jnp.bfloat16, jnp.float32, jnp.int32
NT = (((1,), (1,)), ((), ()))
TN = (((0,), (0,)), ((), ()))
CAP = 16
AXES = ((0, 1, 2), (1, 2, 0), (2, 0, 1))


class Plan:
    def __init__(self, n, half, ff, top, tiles, step):
        self.n, self.half, self.ff, self.top, self.step = n, half, ff, top, step
        self.part = (half + 128) // 3
        self.wide = 3 * self.part
        self.widths = (self.part, self.part, self.part - 128)
        far = lambda d: tuple(min(v, n - v) for v in d)
        self.order = sorted(itertools.product(range(n), repeat=3), key=lambda d: (max(far(d)), sum(d) % 2, d))
        self.slot = {d: i for i, d in enumerate(self.order)}
        self.tiles, start = [], 0
        for count in tiles:
            self.tiles.append((start, count))
            start += count
        self.most = max(tiles)
        self.tile = [t for t, count in enumerate(tiles) for _ in range(count)]
        self.offsets = sorted(range(1, n), key=lambda o: min(o, n - o))
        self.planes = n * n
        self.peers = [d for d in self.order if 0 < sum(v > 0 for v in d) < 3]

    def along(self, f, values):
        out = [0, 0, 0]
        for axis, value in zip(AXES[f], values):
            out[axis] = value
        return tuple(out)

    def seen(self, f, d):
        return tuple(d[axis] for axis in AXES[f])


def kernel(p, ids_ref, cw_ref, go_ref, sg_ref, su_ref, gw_ref, uw_ref, dn_ref, gt_ref, gc_ref,
           xo, s0, s1, s2, r0, r1, r2, g0, g1, g2, gm, ts, tr, gcs, gcr, codes, cws, meta,
           dna, dnb, gwa, gwb, uwa, uwb, sgt, sut, gbuf, pout, pin, hout, hin,
           wsem, wss, wsr, s1s, s1r, ds, dr, ps, pr, hs, hr, rs, rr, tss, trs, sas):
    n, half, part, planes = p.n, p.half, p.part, p.planes
    send, back, gath = (s0, s1, s2), (r0, r1, r2), (g0, g1, g2)
    me, core = lax.axis_index("expert"), lax.axis_index("etp")
    at = (me // (n * n), lax.rem(me // n, n), lax.rem(me, n))
    stride = (n * n, n, 1)

    def device(d, sign=1):
        c = [lax.rem(v + (sign * o) % n, n) for v, o in zip(at, d)]
        return (c[0] * stride[0] + c[1] * stride[1] + c[2], core)

    partner = (me, 1 - core)

    def block_of(d):
        return device(d, -1)[0]

    own = pl.multiple_of(core * half, 128)
    other = pl.multiple_of((1 - core) * half, 128)
    loads = [
        pltpu.make_async_copy(dn_ref.at[:, :, pl.ds(own, half)], dna, wsem.at[0]),
        pltpu.make_async_copy(gw_ref.at[:, pl.ds(own, half), :], gwa, wsem.at[1]),
        pltpu.make_async_copy(uw_ref.at[:, pl.ds(own, half), :], uwa, wsem.at[2]),
    ]
    for load in loads:
        load.start()
    trades = [
        pltpu.make_async_remote_copy(
            src_ref=src, dst_ref=dst, send_sem=wss.at[i], recv_sem=wsr.at[i],
            device_id=partner, device_id_type=MESH)
        for i, (src, dst) in enumerate((
            (dn_ref.at[:, :, pl.ds(other, half)], dnb),
            (gw_ref.at[:, pl.ds(other, half), :], gwb),
            (uw_ref.at[:, pl.ds(other, half), :], uwb),
        ))
    ]

    def saved_start(t):
        first, count = p.tiles[t]
        for j in range(count):
            b = block_of(p.order[first + j])
            pltpu.make_async_copy(sg_ref.at[b], sgt.at[j], sas.at[0]).start()
            pltpu.make_async_copy(su_ref.at[b], sut.at[j], sas.at[1]).start()

    def saved_wait(t):
        count = p.tiles[t][1]
        pltpu.make_async_copy(sg_ref.at[pl.ds(0, count)], sgt.at[pl.ds(0, count)], sas.at[0]).wait()
        pltpu.make_async_copy(su_ref.at[pl.ds(0, count)], sut.at[pl.ds(0, count)], sas.at[1]).wait()

    saved_start(0)

    barrier = pltpu.get_barrier_semaphore()
    for d in p.peers:
        pl.semaphore_signal(barrier, inc=1, device_id=device(d), device_id_type=MESH)
    pl.semaphore_signal(barrier, inc=1, device_id=partner, device_id_type=MESH)

    meta[...] = jnp.concatenate(
        [ids_ref[...].astype(F32), cw_ref[...].astype(F32)], axis=0
    ).astype(BF16)
    tokens = meta.shape[1]
    before = (
        lax.broadcasted_iota(I32, (tokens, tokens), 0)
        < lax.broadcasted_iota(I32, (tokens, tokens), 1)
    ).astype(F32).astype(BF16)
    rows = 2 * planes
    r_iota = lax.broadcasted_iota(I32, (rows, tokens), 0)

    def experts_of(f):
        a, b, c = AXES[f]
        place = r_iota // 2
        vb = lax.rem(at[b] + place // n, n)
        vc = lax.rem(at[c] + lax.rem(place, n), n)
        return 2 * (at[a] * stride[a] + vb * stride[b] + vc * stride[c]) + lax.rem(r_iota, 2)

    experts = [experts_of(f).astype(F32) for f in range(3)]
    c_iota = lax.broadcasted_iota(I32, (rows, CAP, tokens), 1).astype(F32)

    def select(f, a, info, token_cols):
        info = info.astype(F32)
        match = jnp.zeros((rows, tokens), F32)
        weight = jnp.zeros((rows, tokens), F32)
        for k in range(p.top):
            hit = experts[f] == info[k:k + 1, :]
            match = jnp.where(hit, 1.0, match)
            weight = jnp.where(hit, info[p.top + k:p.top + k + 1, :], weight)
        position = jnp.dot(match.astype(BF16), before, preferred_element_type=F32)
        code = jnp.where(match > 0, position, -1.0)
        codes[f, a] = code
        cws[f, a] = weight
        hot = jnp.where(code[:, None, :] == c_iota, 1.0, 0.0)
        hot = hot.reshape(rows * CAP, tokens).astype(BF16)
        width = p.widths[f]
        own_slot = p.slot[p.along(f, (a, 0, 0))]
        for lo in range(0, width, 256):
            hi = min(lo + 256, width)
            picked = jnp.dot(hot, token_cols(lo, hi), preferred_element_type=F32).astype(BF16)
            picked = picked.reshape(planes, 2, CAP, hi - lo)
            send[f][a, :, :, :, lo:hi] = picked
            xo[own_slot, :, :, f * part + lo:f * part + hi] = picked[0]

    def dispatch_copy(f, a, q):
        b, c = q // n, q % n
        width = p.widths[f]
        slot = p.slot[p.along(f, (a, b, c))]
        return pltpu.make_async_remote_copy(
            src_ref=send[f].at[a, q],
            dst_ref=xo.at[slot, :, :, pl.ds(f * part, width)],
            send_sem=ds.at[f, p.tile[slot], a],
            recv_sem=dr.at[f, slot],
            device_id=device(p.along(f, (0, b, c))),
            device_id_type=MESH,
        )

    def gather_copies(f, o):
        to = device(p.along(f, (o, 0, 0)))
        return (
            pltpu.make_async_remote_copy(
                src_ref=go_ref.at[:, pl.ds(f * part, p.widths[f])],
                dst_ref=gath[f].at[o - 1],
                send_sem=s1s.at[f, o - 1, 0], recv_sem=s1r.at[f, o - 1, 0],
                device_id=to, device_id_type=MESH),
            pltpu.make_async_remote_copy(
                src_ref=meta, dst_ref=gm.at[f, o - 1],
                send_sem=s1s.at[f, o - 1, 1], recv_sem=s1r.at[f, o - 1, 1],
                device_id=to, device_id_type=MESH),
        )

    def dispatch(f, a, t):
        return [q for q in range(1, planes)
                if p.tile[p.slot[p.along(f, (a, q // n, q % n))]] == t]

    def dispatch_start(f, a, t):
        for q in dispatch(f, a, t):
            dispatch_copy(f, a, q).start()

    def dispatch_sent(f, a, t):
        k = len(dispatch(f, a, t))
        if k:
            pltpu.make_async_remote_copy(
                src_ref=send[f].at[a, pl.ds(0, k)], dst_ref=send[f].at[a, pl.ds(0, k)],
                send_sem=ds.at[f, t, a], recv_sem=dr.at[f, 0],
                device_id=partner, device_id_type=MESH).wait_send()

    def return_copy(f, t, slot):
        a, b, c = p.seen(f, p.order[slot])
        return pltpu.make_async_remote_copy(
            src_ref=xo.at[slot, :, :, pl.ds(f * part, part)],
            dst_ref=back[f].at[a, b * n + c],
            send_sem=rs.at[f, t], recv_sem=rr.at[f, a],
            device_id=device(p.along(f, (0, b, c)), -1), device_id_type=MESH)

    last = len(p.tiles) - 1
    pl.semaphore_wait(barrier, len(p.peers) + 1)
    for o in p.offsets:
        for f in range(3):
            for copy in gather_copies(f, o):
                copy.start()
    for trade in trades:
        trade.start()
    for f in range(3):
        select(f, 0, meta[...], lambda lo, hi: go_ref[:, f * part + lo:f * part + hi])
        dispatch_start(f, 0, 0)
    for a in p.offsets:
        for f in range(3):
            for copy in gather_copies(f, a):
                copy.wait_recv()
            select(f, a, gm[f, a - 1], lambda lo, hi: gath[f][a - 1, :, lo:hi])
            dispatch_start(f, a, 0)
    for a in [0] + p.offsets:
        for f in range(3):
            dispatch_sent(f, a, 0)
            if last >= 1:
                dispatch_start(f, a, 1)

    for t, (first, count) in enumerate(p.tiles):
        m = count * CAP
        for slot in range(first, first + count):
            for f in range(3):
                a, b, c = p.seen(f, p.order[slot])
                if (b, c) != (0, 0):
                    dispatch_copy(f, a, b * n + c).wait_recv()
        if t == 0:
            loads[0].wait()
            trades[0].wait_recv()

        def part_copy(l):
            return pltpu.make_async_remote_copy(
                src_ref=pout.at[l, pl.ds(0, m)], dst_ref=pin.at[l, pl.ds(0, m)],
                send_sem=ps.at[l], recv_sem=pr.at[l], device_id=partner, device_id_type=MESH)

        def hidden_copy(l):
            return pltpu.make_async_remote_copy(
                src_ref=hout.at[l, pl.ds(0, m)], dst_ref=hin.at[l, pl.ds(0, m)],
                send_sem=hs.at[l], recv_sem=hr.at[l], device_id=partner, device_id_type=MESH)

        def features(l):
            return xo[pl.ds(first, count), l, :, 0:half].reshape(m, half)

        def part_of_other(l, _):
            pout[l, 0:m, :] = lax.dot_general(features(l), dnb[l], NT, preferred_element_type=F32)
            part_copy(l).start()
            return 0

        def part_of_own(l, _):
            gbuf[l, 0:m, :] = lax.dot_general(features(l), dna[l], NT, preferred_element_type=F32)
            return 0

        def pointwise(l, at_row, j):
            grad = gbuf[l, at_row, :] + pin[l, at_row, :]
            gate = sgt[j, l].astype(F32)
            up = sut[j, l].astype(F32)
            sig = 0.5 * jnp.tanh(0.5 * gate) + 0.5
            act = gate * sig
            gup = grad * act
            total = jnp.sum(gup * up, axis=1, keepdims=True)
            hout[l, at_row, 0:p.ff] = (grad * up * sig * (1.0 + gate * (1.0 - sig))).astype(BF16)
            hout[l, at_row, p.ff:2 * p.ff] = gup.astype(BF16)
            hout[l, at_row, 2 * p.ff:] = jnp.broadcast_to(total, (CAP, 128)).astype(BF16)

        def hidden(l, _):
            part_copy(l).wait_recv()

            def two(i, _):
                for k in range(2):
                    j = 2 * i + k
                    pointwise(l, pl.ds(pl.multiple_of(j * CAP, CAP), CAP), j)
                return 0

            lax.fori_loop(0, count // 2, two, 0)
            if count % 2:
                pointwise(l, pl.ds((count - 1) * CAP, CAP), count - 1)
            hidden_copy(l).start()
            return 0

        def project(l, _):
            hidden_copy(l).wait_recv()
            sums = hout[l, 0:m, 2 * p.ff:].astype(F32) + hin[l, 0:m, 2 * p.ff:].astype(F32)
            xo[pl.ds(first, count), l, :, half:half + 128] = sums.astype(BF16).reshape(count, CAP, 128)
            for lo in range(0, half, p.step):
                u = None
                for h, gate_w, up_w in ((hout, gwa, uwa), (hin, gwb, uwb)):
                    for at_col, w in ((0, gate_w), (p.ff, up_w)):
                        term = lax.dot_general(
                            h[l, 0:m, at_col:at_col + p.ff], w[l, lo:lo + p.step, :], NT,
                            preferred_element_type=F32)
                        u = term if u is None else u + term
                xo[pl.ds(first, count), l, :, lo:lo + p.step] = u.astype(BF16).reshape(count, CAP, p.step)
            return 0

        def sent(copy):
            def wait(l, _):
                copy(l).wait_send()
                return 0
            lax.fori_loop(0, 2, wait, 0)

        lax.fori_loop(0, 2, part_of_other, 0)
        lax.fori_loop(0, 2, part_of_own, 0)
        saved_wait(t)
        lax.fori_loop(0, 2, hidden, 0)
        if t < last:
            saved_start(t + 1)
        if t == 0:
            for load in loads[1:]:
                load.wait()
            for trade in trades[1:]:
                trade.wait_recv()
        if 0 < t + 2 <= last:
            for a in [0] + p.offsets:
                for f in range(3):
                    dispatch_start(f, a, t + 2)
        lax.fori_loop(0, 2, project, 0)
        sent(part_copy)
        sent(hidden_copy)
        for slot in range(first, first + count):
            for f in range(3):
                a, b, c = p.seen(f, p.order[slot])
                if (b, c) == (0, 0):
                    back[f][a, 0] = xo[slot, :, :, f * part:(f + 1) * part]
                else:
                    return_copy(f, t, slot).start()

    def total_copy(f, o):
        to = device(p.along(f, (o, 0, 0)), -1)
        width = p.widths[f]
        copies = [pltpu.make_async_remote_copy(
            src_ref=ts.at[f, o - 1, :, pl.ds(0, width)], dst_ref=tr.at[f, o - 1, :, pl.ds(0, width)],
            send_sem=tss.at[f, o - 1, 0], recv_sem=trs.at[f, o - 1, 0],
            device_id=to, device_id_type=MESH)]
        if f == 2:
            copies.append(pltpu.make_async_remote_copy(
                src_ref=gcs.at[o - 1], dst_ref=gcr.at[o - 1],
                send_sem=tss.at[f, o - 1, 1], recv_sem=trs.at[f, o - 1, 1],
                device_id=to, device_id_type=MESH))
        return copies

    def back_wait(f, a):
        pltpu.make_async_remote_copy(
            src_ref=xo.at[pl.ds(0, planes - 1), :, :, pl.ds(0, part)],
            dst_ref=back[f].at[a, pl.ds(1, planes - 1)],
            send_sem=rs.at[f, 0], recv_sem=rr.at[f, a],
            device_id=partner, device_id_type=MESH).wait_recv()

    def combined(f, a, info):
        back_wait(f, a)
        hit = codes[f, a][:, None, :] == c_iota
        weight = jnp.where(hit, cws[f, a][:, None, :], 0.0)
        weight = weight.reshape(rows * CAP, tokens).astype(BF16)
        width = p.widths[f]
        values = back[f][a, :, :, :, 0:width].reshape(rows * CAP, width)
        total = lax.dot_general(weight, values, TN, preferred_element_type=F32)
        if f < 2:
            return total, None
        hot = jnp.where(hit, 1.0, 0.0).reshape(rows * CAP, tokens).astype(BF16)
        sums = back[f][a, :, :, :, width:part].reshape(rows * CAP, 128)
        lane = lax.broadcasted_iota(I32, (rows * CAP, 128), 1)
        row = lax.broadcasted_iota(I32, (rows * CAP, 128), 0) // CAP
        sums = jnp.where(lane == row, sums.astype(F32), 0.0).astype(BF16)
        spread = lax.dot_general(sums, hot, TN, preferred_element_type=F32)[0:rows]
        info = info.astype(F32)
        picked = [
            jnp.sum(jnp.where(experts[f] == info[k:k + 1, :], spread, 0.0), axis=0, keepdims=True)
            for k in range(p.top)
        ]
        return total, jnp.concatenate(picked, axis=0)

    for a in p.offsets:
        for f in range(3):
            total, sums = combined(f, a, gm[f, a - 1])
            ts[f, a - 1, :, 0:p.widths[f]] = total.astype(BF16)
            if f == 2:
                gcs[a - 1] = sums
            for copy in total_copy(f, a):
                copy.start()
    for f in range(3):
        total, sums = combined(f, 0, meta[...])
        width = p.widths[f]
        for a in range(1, n):
            for copy in total_copy(f, a):
                copy.wait_recv()
            total = total + tr[f, a - 1, :, 0:width].astype(F32)
            if f == 2:
                sums = sums + gcr[a - 1]
        gt_ref[:, f * part:f * part + width] = total.astype(BF16)
        if f == 2:
            gc_ref[...] = sums.astype(BF16)

    for f in range(3):
        width = p.widths[f]
        for o in range(1, n):
            for copy in gather_copies(f, o) + tuple(total_copy(f, o)):
                copy.wait_send()
        for t, (first, count) in enumerate(p.tiles):
            if t > 0:
                for a in range(n):
                    dispatch_sent(f, a, t)
            sent = sum(p.seen(f, p.order[s])[1:] != (0, 0) for s in range(first, first + count))
            if sent:
                pltpu.make_async_remote_copy(
                    src_ref=xo.at[pl.ds(0, sent), :, :, pl.ds(0, part)],
                    dst_ref=xo.at[pl.ds(0, sent), :, :, pl.ds(0, part)],
                    send_sem=rs.at[f, t], recv_sem=rr.at[f, 0],
                    device_id=partner, device_id_type=MESH).wait_send()
    for trade in trades:
        trade.wait_send()


def on_device(plan, grad_out, combine, expert_ids, saved_gate, saved_up, gate_weight, up_weight, down_weight):
    p = plan
    n, half, ff, part, planes = p.n, p.half, p.ff, p.part, p.planes
    tokens, top = expert_ids.shape
    blocks, nt = n * n * n, len(p.tiles)
    saved = [
        jnp.transpose(v.reshape(blocks, CAP, 2, ff), (0, 2, 1, 3)) for v in (saved_gate, saved_up)
    ]
    vmem = pl.BlockSpec(memory_space=pltpu.VMEM)
    hbm = pl.BlockSpec(memory_space=pl.ANY)
    dma = pltpu.SemaphoreType.DMA
    rows = 2 * planes
    scratch = [
        pltpu.VMEM((blocks, 2, CAP, p.wide), BF16),
        *[pltpu.VMEM((n, planes, 2, CAP, w), BF16) for w in p.widths],
        *[pltpu.VMEM((n, planes, 2, CAP, part), BF16) for _ in range(3)],
        *[pltpu.VMEM((n - 1, tokens, w), BF16) for w in p.widths],
        pltpu.VMEM((3, n - 1, 2 * top, tokens), BF16),
        pltpu.VMEM((3, n - 1, tokens, part), BF16),
        pltpu.VMEM((3, n - 1, tokens, part), BF16),
        pltpu.VMEM((n - 1, top, tokens), F32),
        pltpu.VMEM((n - 1, top, tokens), F32),
        pltpu.VMEM((3, n, rows, tokens), F32),
        pltpu.VMEM((3, n, rows, tokens), F32),
        pltpu.VMEM((2 * top, tokens), BF16),
        pltpu.VMEM((2, ff, half), BF16),
        pltpu.VMEM((2, ff, half), BF16),
        *[pltpu.VMEM((2, half, ff), BF16) for _ in range(4)],
        pltpu.VMEM((p.most, 2, CAP, ff), BF16),
        pltpu.VMEM((p.most, 2, CAP, ff), BF16),
        *[pltpu.VMEM((2, p.most * CAP, ff), F32) for _ in range(3)],
        *[pltpu.VMEM((2, p.most * CAP, 2 * ff + 128), BF16) for _ in range(2)],
        dma((3,)), dma((3,)), dma((3,)), dma((3, n - 1, 2)), dma((3, n - 1, 2)),
        dma((3, nt, n)), dma((3, blocks)), dma((2,)), dma((2,)), dma((2,)), dma((2,)),
        dma((3, nt)), dma((3, n)), dma((3, n - 1, 2)), dma((3, n - 1, 2)), dma((2,)),
    ]
    grad_tokens, grad_combine = pl.pallas_call(
        functools.partial(kernel, p),
        out_shape=(
            jax.ShapeDtypeStruct((tokens, half), BF16),
            jax.ShapeDtypeStruct((top, tokens), BF16),
        ),
        in_specs=[vmem, vmem, vmem, hbm, hbm, hbm, hbm, hbm],
        out_specs=(vmem, vmem),
        scratch_shapes=scratch,
        compiler_params=pltpu.CompilerParams(
            collective_id=0, has_side_effects=True, vmem_limit_bytes=67043328
        ),
    )(expert_ids.T, combine.T, grad_out, *saved, gate_weight, up_weight, down_weight)
    return grad_tokens, grad_combine.T


def solution(mesh, tiles=(27, 19, 18), step=256):
    n = round(mesh.shape["expert"] ** (1 / 3))

    def run(grad_out, combine, expert_ids, saved_gate, saved_up, gate_weight, up_weight, down_weight):
        plan = Plan(n, grad_out.shape[1], gate_weight.shape[2], expert_ids.shape[1], tiles, step)
        return on_device(
            plan, grad_out, combine, expert_ids, saved_gate, saved_up, gate_weight, up_weight, down_weight
        )

    in_specs = (
        P("expert", "etp"),
        P("expert", None),
        P("expert", None),
        P(None, "expert", "etp"),
        P(None, "expert", "etp"),
        P("expert", None, "etp"),
        P("expert", None, "etp"),
        P("expert", "etp", None),
    )
    out_specs = (P("expert", "etp"), P("expert", None))
    return jax.shard_map(run, mesh=mesh, in_specs=in_specs, out_specs=out_specs, check_vma=False)
```

```python
import functools
import itertools

import jax
import jax.numpy as jnp
from jax import lax
from jax.experimental import pallas as pl
from jax.experimental.pallas import tpu as pltpu
from jax.sharding import PartitionSpec as P

MESH = pl.DeviceIdType.MESH
BF16, F32, I32 = jnp.bfloat16, jnp.float32, jnp.int32
NT = (((1,), (1,)), ((), ()))
TN = (((0,), (0,)), ((), ()))
CAP = 16
AXES = ((0, 1, 2), (1, 2, 0), (2, 0, 1))


class Plan:
    def __init__(self, n, half, ff, top, tiles, step):
        self.n, self.half, self.ff, self.top, self.step = n, half, ff, top, step
        self.part = (half + 128) // 3
        self.base = (0, self.part, 2 * self.part - 128)
        far = lambda d: tuple(min(v, n - v) for v in d)
        self.order = sorted(itertools.product(range(n), repeat=3), key=lambda d: (max(far(d)), sum(d) % 2, d))
        self.slot = {d: i for i, d in enumerate(self.order)}
        self.tiles, start = [], 0
        for count in tiles:
            self.tiles.append((start, count))
            start += count
        self.most = max(tiles)
        self.tile = [t for t, count in enumerate(tiles) for _ in range(count)]
        self.offsets = sorted(range(1, n), key=lambda o: min(o, n - o))
        self.planes = n * n
        self.kind, load = {}, [0, 0, 0]
        for d in sorted(self.order, key=lambda d: -sum(far(d))):
            choices = []
            for kind in range(2):
                new = list(load)
                for f in range(3):
                    lo, hi = self.span_of(f, kind)
                    for axis in AXES[f][1:]:
                        new[axis] += (hi - lo) * far(d)[axis]
                choices.append((max(new), kind, new))
            _, self.kind[d], load = min(choices)
        self.peers = [d for d in self.order if 0 < sum(v > 0 for v in d) < 3]

    def span_of(self, f, kind):
        lo, hi = self.base[f], self.base[f] + self.part
        return (lo + 128 if (f, kind) == (2, 0) else lo, hi - 128 if (f, kind) == (1, 1) else hi)

    def span(self, f, d):
        return self.span_of(f, self.kind[d])

    def along(self, f, values):
        out = [0, 0, 0]
        for axis, value in zip(AXES[f], values):
            out[axis] = value
        return tuple(out)

    def seen(self, f, d):
        return tuple(d[axis] for axis in AXES[f])


def kernel(p, ids_ref, cw_ref, go_ref, sg_ref, su_ref, gw_ref, uw_ref, dn_ref, gt_ref, gc_ref,
           xo, s0, s1, s2, r0, r1, r2, g0, g1, g2, gm, ts, tr, gcs, gcr, codes, cws, meta,
           dna, dnb, gwa, gwb, uwa, uwb, sgt, sut, gbuf, pout, pin, hout, hin, dws, dwr,
           wsem, wss, wsr, s1s, s1r, ds, dr, ps, pr, hs, hr, rs, rr, tss, trs, sas, es, er, pace):
    n, half, part, planes = p.n, p.half, p.part, p.planes
    send, back, gath = (s0, s1, s2), (r0, r1, r2), (g0, g1, g2)
    me, core = lax.axis_index("expert"), lax.axis_index("etp")
    at = (me // (n * n), lax.rem(me // n, n), lax.rem(me, n))
    stride = (n * n, n, 1)

    def device(d, sign=1):
        c = [lax.rem(v + (sign * o) % n, n) for v, o in zip(at, d)]
        return (c[0] * stride[0] + c[1] * stride[1] + c[2], core)

    partner = (me, 1 - core)

    def block_of(d):
        return device(d, -1)[0]

    own = pl.multiple_of(core * half, 128)
    other = pl.multiple_of((1 - core) * half, 128)
    loads = [
        pltpu.make_async_copy(dn_ref.at[:, :, pl.ds(own, half)], dna, wsem.at[0]),
        pltpu.make_async_copy(gw_ref.at[:, pl.ds(own, half), :], gwa, wsem.at[1]),
        pltpu.make_async_copy(uw_ref.at[:, pl.ds(own, half), :], uwa, wsem.at[2]),
    ]
    for load in loads:
        load.start()
    trades = [
        pltpu.make_async_remote_copy(
            src_ref=src, dst_ref=dst, send_sem=wss.at[i], recv_sem=wsr.at[i],
            device_id=partner, device_id_type=MESH)
        for i, (src, dst) in enumerate((
            (dn_ref.at[:, :, pl.ds(other, half)], dnb),
            (gw_ref.at[:, pl.ds(other, half), :], gwb),
            (uw_ref.at[:, pl.ds(other, half), :], uwb),
        ))
    ]

    def saved_start(t):
        first, count = p.tiles[t]
        for j in range(count):
            b = block_of(p.order[first + j])
            block = pl.ds(pl.multiple_of(b * CAP, CAP), CAP)
            rows_at = pl.ds(j * CAP, CAP)
            pltpu.make_async_copy(sg_ref.at[block], sgt.at[rows_at], sas.at[0]).start()
            pltpu.make_async_copy(su_ref.at[block], sut.at[rows_at], sas.at[1]).start()

    def saved_wait(t):
        count = p.tiles[t][1] * CAP
        pltpu.make_async_copy(sg_ref.at[pl.ds(0, count)], sgt.at[pl.ds(0, count)], sas.at[0]).wait()
        pltpu.make_async_copy(su_ref.at[pl.ds(0, count)], sut.at[pl.ds(0, count)], sas.at[1]).wait()

    saved_start(0)

    for f in (1, 2):
        for a in range(n):
            for q in range(planes):
                kind = p.kind[p.along(f, (a, q // n, q % n))]
                if f == 1 and kind == 1:
                    back[f][a, q, :, :, part - 128:part] = jnp.zeros((2, CAP, 128), BF16)
                if f == 2 and kind == 0:
                    back[f][a, q, :, :, 0:128] = jnp.zeros((2, CAP, 128), BF16)

    barrier = pltpu.get_barrier_semaphore()
    for d in p.peers:
        pl.semaphore_signal(barrier, inc=1, device_id=device(d), device_id_type=MESH)
    pl.semaphore_signal(barrier, inc=1, device_id=partner, device_id_type=MESH)

    meta[...] = jnp.concatenate(
        [ids_ref[...].astype(F32), cw_ref[...].astype(F32)], axis=0
    ).astype(BF16)
    tokens = meta.shape[1]
    before = (
        lax.broadcasted_iota(I32, (tokens, tokens), 0)
        < lax.broadcasted_iota(I32, (tokens, tokens), 1)
    ).astype(F32).astype(BF16)
    rows = 2 * planes
    r_iota = lax.broadcasted_iota(I32, (rows, tokens), 0)

    def experts_of(f, place, which):
        a, b, c = AXES[f]
        vb = lax.rem(at[b] + place // n, n)
        vc = lax.rem(at[c] + lax.rem(place, n), n)
        return 2 * (at[a] * stride[a] + vb * stride[b] + vc * stride[c]) + which

    experts = [experts_of(f, r_iota // 2, lax.rem(r_iota, 2)).astype(F32) for f in range(3)]
    c_iota = lax.broadcasted_iota(I32, (rows, CAP, tokens), 1).astype(F32)

    def select(f, a, info, token_cols):
        info = info.astype(F32)
        match = jnp.zeros((rows, tokens), F32)
        weight = jnp.zeros((rows, tokens), F32)
        for k in range(p.top):
            hit = experts[f] == info[k:k + 1, :]
            match = jnp.where(hit, 1.0, match)
            weight = jnp.where(hit, info[p.top + k:p.top + k + 1, :], weight)
        position = jnp.dot(match.astype(BF16), before, preferred_element_type=F32)
        code = jnp.where(match > 0, position, -1.0)
        codes[f, a] = code
        cws[f, a] = weight
        hot = jnp.where(code[:, None, :] == c_iota, 1.0, 0.0)
        hot = hot.reshape(rows * CAP, tokens).astype(BF16)
        own_place = p.along(f, (a, 0, 0))
        own_slot, own_span = p.slot[own_place], p.span(f, own_place)
        for lo in range(0, part, 256):
            hi = min(lo + 256, part)
            picked = jnp.dot(hot, token_cols(lo, hi), preferred_element_type=F32).astype(BF16)
            picked = picked.reshape(planes, 2, CAP, hi - lo)
            send[f][a, :, :, :, lo:hi] = picked
            x_lo, x_hi = max(p.base[f] + lo, own_span[0]), min(p.base[f] + hi, own_span[1])
            if x_lo < x_hi:
                at_col = x_lo - p.base[f] - lo
                xo[own_slot, :, :, x_lo:x_hi] = picked[0, :, :, at_col:at_col + x_hi - x_lo]

    def dispatch_copy(f, a, q):
        b, c = q // n, q % n
        place = p.along(f, (a, b, c))
        slot, (lo, hi) = p.slot[place], p.span(f, place)
        return pltpu.make_async_remote_copy(
            src_ref=send[f].at[a, q, :, :, pl.ds(lo - p.base[f], hi - lo)],
            dst_ref=xo.at[slot, :, :, pl.ds(lo, hi - lo)],
            send_sem=ds.at[f, p.tile[slot], a],
            recv_sem=dr.at[f, slot],
            device_id=device(p.along(f, (0, b, c))),
            device_id_type=MESH,
        )

    def gather_copies(f, o):
        to = device(p.along(f, (o, 0, 0)))
        return (
            pltpu.make_async_remote_copy(
                src_ref=go_ref.at[:, pl.ds(p.base[f], part)],
                dst_ref=gath[f].at[o - 1],
                send_sem=s1s.at[f, o - 1, 0], recv_sem=s1r.at[f, o - 1, 0],
                device_id=to, device_id_type=MESH),
            pltpu.make_async_remote_copy(
                src_ref=meta, dst_ref=gm.at[f, o - 1],
                send_sem=s1s.at[f, o - 1, 1], recv_sem=s1r.at[f, o - 1, 1],
                device_id=to, device_id_type=MESH),
        )

    def dispatch(f, a, t):
        return [q for q in range(1, planes)
                if p.tile[p.slot[p.along(f, (a, q // n, q % n))]] == t]

    def dispatch_start(f, a, t):
        for q in dispatch(f, a, t):
            dispatch_copy(f, a, q).start()

    def bytes_of(spans, sem):
        lanes = min(256, p.ff)
        size = sum(hi - lo for lo, hi in spans) * 2 * CAP // lanes
        rows_at = gwa.at[0, pl.ds(0, size), pl.ds(0, lanes)]
        return pltpu.make_async_remote_copy(
            src_ref=rows_at, dst_ref=rows_at, send_sem=sem, recv_sem=sem,
            device_id=partner, device_id_type=MESH)

    def drain_sent(spans, sem):
        if spans:
            bytes_of(spans, sem).wait_send()

    def dispatch_sent(f, a, t):
        drain_sent([p.span(f, p.along(f, (a, q // n, q % n))) for q in dispatch(f, a, t)], ds.at[f, t, a])

    def group(a):
        return min(a, n - a)

    def returns(f, t, g):
        first, count = p.tiles[t]
        found = [(slot, p.seen(f, p.order[slot])) for slot in range(first, first + count)]
        return [(slot, d) for slot, d in found if group(d[0]) == g]

    def return_copy(f, t, slot):
        a, b, c = p.seen(f, p.order[slot])
        lo, hi = p.span(f, p.order[slot])
        return pltpu.make_async_remote_copy(
            src_ref=xo.at[slot, :, :, pl.ds(lo, hi - lo)],
            dst_ref=back[f].at[a, b * n + c, :, :, pl.ds(lo - p.base[f], hi - lo)],
            send_sem=rs.at[f, t, group(a)], recv_sem=rr.at[f, a],
            device_id=device(p.along(f, (0, b, c)), -1), device_id_type=MESH)

    def weight_copy(slot):
        a, b, c = p.seen(2, p.order[slot])
        return pltpu.make_async_remote_copy(
            src_ref=dws.at[slot], dst_ref=dwr.at[a, b * n + c], send_sem=es.at[0], recv_sem=er.at[a],
            device_id=device(p.along(2, (0, b, c)), -1), device_id_type=MESH)

    def return_start(t, g):
        lists = [returns(f, t, g) for f in range(3)]
        for i in range(max(len(v) for v in lists)):
            for f in range(3):
                if i < len(lists[f]):
                    slot, (a, b, c) = lists[f][i]
                    if (b, c) == (0, 0):
                        lo, hi = p.span(f, p.order[slot])
                        back[f][a, 0, :, :, lo - p.base[f]:hi - p.base[f]] = xo[slot, :, :, lo:hi]
                        if f == 2:
                            dwr[a, 0] = dws[slot]
                    else:
                        if f == 2:
                            weight_copy(slot).start()
                        return_copy(f, t, slot).start()

    def return_sent(t, g):
        for f in range(3):
            drain_sent([p.span(f, p.order[slot]) for slot, d in returns(f, t, g) if d[1:] != (0, 0)],
                       rs.at[f, t, g])

    last = len(p.tiles) - 1
    pl.semaphore_wait(barrier, len(p.peers) + 1)
    for o in p.offsets:
        for f in range(3):
            for copy in gather_copies(f, o):
                copy.start()
    trades[0].start()
    for f in range(3):
        select(f, 0, meta[...], lambda lo, hi: go_ref[:, p.base[f] + lo:p.base[f] + hi])
        dispatch_start(f, 0, 0)
    for a in p.offsets:
        for f in range(3):
            for copy in gather_copies(f, a):
                copy.wait_recv()
            select(f, a, gm[f, a - 1], lambda lo, hi: gath[f][a - 1, :, lo:hi])
            dispatch_start(f, a, 0)
    for a in [0] + p.offsets:
        for f in range(3):
            dispatch_sent(f, a, 0)
    pl.semaphore_signal(pace, inc=1, device_id=partner, device_id_type=MESH)
    pl.semaphore_wait(pace, 1)
    if last >= 1:
        for a in [0] + p.offsets:
            for f in range(3):
                dispatch_start(f, a, 1)
    for trade in trades[1:]:
        trade.start()
    for t, (first, count) in enumerate(p.tiles):
        m = count * CAP
        for slot in range(first, first + count):
            for f in range(3):
                a, b, c = p.seen(f, p.order[slot])
                if (b, c) != (0, 0):
                    dispatch_copy(f, a, b * n + c).wait_recv()
        if t == 0:
            loads[0].wait()
            trades[0].wait_recv()

        def part_copy(l):
            return pltpu.make_async_remote_copy(
                src_ref=pout.at[l, pl.ds(0, m)], dst_ref=pin.at[l, pl.ds(0, m)],
                send_sem=ps.at[l], recv_sem=pr.at[l], device_id=partner, device_id_type=MESH)

        def hidden_copy(l):
            return pltpu.make_async_remote_copy(
                src_ref=hout.at[l, pl.ds(0, m)], dst_ref=hin.at[l, pl.ds(0, m)],
                send_sem=hs.at[l], recv_sem=hr.at[l], device_id=partner, device_id_type=MESH)

        def features(l):
            return xo[pl.ds(first, count), l, :, 0:half].reshape(m, half)

        def part_of_other(l, _):
            pout[l, 0:m, :] = lax.dot_general(features(l), dnb[l], NT, preferred_element_type=F32)
            part_copy(l).start()
            return 0

        def part_of_own(l, _):
            gbuf[l, 0:m, :] = lax.dot_general(features(l), dna[l], NT, preferred_element_type=F32)
            return 0

        def pointwise(l, j):
            at_row = pl.ds(pl.multiple_of(j * CAP, CAP), CAP)
            grad = gbuf[l, at_row, :] + pin[l, at_row, :]
            gate = jnp.swapaxes(sgt[at_row], 0, 1)[l].astype(F32)
            up = jnp.swapaxes(sut[at_row], 0, 1)[l].astype(F32)
            sig = 0.5 * jnp.tanh(0.5 * gate) + 0.5
            act = gate * sig
            gup = grad * act
            total = jnp.sum(gup * up, axis=1, keepdims=True)
            hout[l, at_row, 0:p.ff] = (grad * up * sig * (1.0 + gate * (1.0 - sig))).astype(BF16)
            hout[l, at_row, p.ff:2 * p.ff] = gup.astype(BF16)
            hout[l, at_row, 2 * p.ff:] = jnp.broadcast_to(total, (CAP, 128)).astype(BF16)

        def hidden():
            for l in range(2):
                part_copy(l).wait_recv()

                def two(i, _):
                    pointwise(l, 2 * i)
                    pointwise(l, 2 * i + 1)
                    return 0

                lax.fori_loop(0, count // 2, two, 0)
                if count % 2:
                    pointwise(l, count - 1)
                hidden_copy(l).start()

        def project(l, _):
            hidden_copy(l).wait_recv()
            for lo in range(0, half, p.step):
                u = None
                for h, gate_w, up_w in ((hout, gwa, uwa), (hin, gwb, uwb)):
                    for at_col, w in ((0, gate_w), (p.ff, up_w)):
                        term = lax.dot_general(
                            h[l, 0:m, at_col:at_col + p.ff], w[l, lo:lo + p.step, :], NT,
                            preferred_element_type=F32)
                        u = term if u is None else u + term
                xo[pl.ds(first, count), l, :, lo:lo + p.step] = u.astype(BF16).reshape(count, CAP, p.step)
            return 0

        def sent(copy):
            def wait(l, _):
                copy(l).wait_send()
                return 0
            lax.fori_loop(0, 2, wait, 0)

        lax.fori_loop(0, 2, part_of_other, 0)
        lax.fori_loop(0, 2, part_of_own, 0)
        saved_wait(t)
        hidden()
        if t < last:
            saved_start(t + 1)
        if t == 0:
            for load in loads[1:]:
                load.wait()
            for trade in trades[1:]:
                trade.wait_recv()
        if 0 < t + 2 <= last:
            for a in [0] + p.offsets:
                for f in range(3):
                    dispatch_start(f, a, t + 2)
        lax.fori_loop(0, 2, project, 0)
        row = None
        for l in range(2):
            sums = hout[l, 0:m, 2 * p.ff:].astype(F32) + hin[l, 0:m, 2 * p.ff:].astype(F32)
            sums = sums.astype(BF16).astype(F32).reshape(count, CAP, 128)
            shape = (count, CAP, 128)
            lane = lax.rem(lax.broadcasted_iota(I32, shape, 2), 2 * CAP)
            mine = lane == l * CAP + lax.broadcasted_iota(I32, shape, 1)
            term = jnp.sum(jnp.where(mine, sums, 0.0), axis=1, keepdims=True)
            row = term if row is None else row + term
        dws[pl.ds(first, count)] = row
        sent(part_copy)
        sent(hidden_copy)
        for g in range(n // 2, 0, -1):
            return_start(t, g)

    def total_copy(f, o):
        to = device(p.along(f, (o, 0, 0)), -1)
        copies = [pltpu.make_async_remote_copy(
            src_ref=ts.at[f, o - 1], dst_ref=tr.at[f, o - 1],
            send_sem=tss.at[f, o - 1, 0], recv_sem=trs.at[f, o - 1, 0],
            device_id=to, device_id_type=MESH)]
        if f == 2:
            copies.append(pltpu.make_async_remote_copy(
                src_ref=gcs.at[o - 1], dst_ref=gcr.at[o - 1],
                send_sem=tss.at[f, o - 1, 1], recv_sem=trs.at[f, o - 1, 1],
                device_id=to, device_id_type=MESH))
        return copies

    def back_wait(f, a):
        spans = [p.span(f, p.along(f, (a, q // n, q % n))) for q in range(1, planes)]
        bytes_of(spans, rr.at[f, a]).wait_recv()
        if f == 2:
            pltpu.make_async_remote_copy(
                src_ref=dwr.at[a, pl.ds(1, planes - 1)], dst_ref=dwr.at[a, pl.ds(1, planes - 1)],
                send_sem=es.at[0], recv_sem=er.at[a],
                device_id=partner, device_id_type=MESH).wait_recv()

    def combined(f, a, info):
        back_wait(f, a)
        hit = codes[f, a][:, None, :] == c_iota
        weight = jnp.where(hit, cws[f, a][:, None, :], 0.0)
        weight = weight.reshape(rows * CAP, tokens).astype(BF16)
        values = back[f][a].reshape(rows * CAP, part)
        total = lax.dot_general(weight, values, TN, preferred_element_type=F32)
        if f < 2:
            return total, None
        hot = jnp.where(hit, 1.0, 0.0).reshape(rows * CAP, tokens).astype(BF16)
        values = dwr[a].reshape(planes, 128)
        wide = jnp.concatenate([values] * (rows * CAP // 128), axis=1)
        wide = jnp.concatenate([wide, wide], axis=0)
        lane = lax.broadcasted_iota(I32, wide.shape, 1)
        line = lax.broadcasted_iota(I32, wide.shape, 0)
        mine = lane // CAP == 2 * lax.rem(line, planes) + line // planes
        wide = jnp.where(mine, wide, 0.0).astype(BF16)
        spread = jnp.dot(wide, hot, preferred_element_type=F32)
        info = info.astype(F32)
        by_choice = experts_of(f, lax.rem(r_iota, planes), r_iota // planes).astype(F32)
        picked = [
            jnp.sum(jnp.where(by_choice == info[k:k + 1, :], spread, 0.0), axis=0, keepdims=True)
            for k in range(p.top)
        ]
        return total, jnp.concatenate(picked, axis=0)

    def partial_sums(a):
        for f in range(3):
            total, sums = combined(f, a, gm[f, a - 1])
            ts[f, a - 1] = total.astype(BF16)
            if f == 2:
                gcs[a - 1] = sums
            for copy in total_copy(f, a):
                copy.start()

    for t in range(last):
        for g in range(1, n // 2 + 1):
            return_sent(t, g)
    if n > 2:
        return_sent(last, n // 2)
    return_start(0, 0)
    for a in p.offsets[::-1]:
        if group(a) == 1 and a == p.offsets[::-1][0 if n == 2 else 1]:
            return_sent(last, 1)
            for t in range(1, last + 1):
                return_start(t, 0)
        partial_sums(a)
    shared = None
    for f in range(3):
        total, sums = combined(f, 0, meta[...])
        for a in range(1, n):
            for copy in total_copy(f, a):
                copy.wait_recv()
            total = total + tr[f, a - 1].astype(F32)
            if f == 2:
                sums = sums + gcr[a - 1]
        lo, hi = 0, part
        if f == 1:
            shared, hi = total[:, part - 128:], part - 128
        if f == 2:
            gt_ref[:, p.base[2]:p.base[2] + 128] = (total[:, 0:128] + shared).astype(BF16)
            gc_ref[...] = sums.astype(BF16)
            lo = 128
        gt_ref[:, p.base[f] + lo:p.base[f] + hi] = total[:, lo:hi].astype(BF16)

    for f in range(3):
        for o in range(1, n):
            for copy in gather_copies(f, o) + tuple(total_copy(f, o)):
                copy.wait_send()
        for t in range(1, last + 1):
            for a in range(n):
                dispatch_sent(f, a, t)
    for t in range(last + 1):
        for g in range(n // 2 + 1):
            if g == 0:
                return_sent(t, g)
    sent_rows = sum(p.seen(2, d)[1:] != (0, 0) for d in p.order)
    pltpu.make_async_remote_copy(
        src_ref=dws.at[pl.ds(0, sent_rows)], dst_ref=dws.at[pl.ds(0, sent_rows)],
        send_sem=es.at[0], recv_sem=er.at[0], device_id=partner, device_id_type=MESH).wait_send()
    for trade in trades:
        trade.wait_send()


def on_device(plan, grad_out, combine, expert_ids, saved_gate, saved_up, gate_weight, up_weight, down_weight):
    p = plan
    n, half, ff, part, planes = p.n, p.half, p.ff, p.part, p.planes
    tokens, top = expert_ids.shape
    blocks, nt = n * n * n, len(p.tiles)
    vmem = pl.BlockSpec(memory_space=pltpu.VMEM)
    hbm = pl.BlockSpec(memory_space=pl.ANY)
    dma = pltpu.SemaphoreType.DMA
    rows = 2 * planes
    scratch = [
        pltpu.VMEM((blocks, 2, CAP, half), BF16),
        *[pltpu.VMEM((n, planes, 2, CAP, part), BF16) for _ in range(6)],
        *[pltpu.VMEM((n - 1, tokens, part), BF16) for _ in range(3)],
        pltpu.VMEM((3, n - 1, 2 * top, tokens), BF16),
        pltpu.VMEM((3, n - 1, tokens, part), BF16),
        pltpu.VMEM((3, n - 1, tokens, part), BF16),
        pltpu.VMEM((n - 1, top, tokens), F32),
        pltpu.VMEM((n - 1, top, tokens), F32),
        pltpu.VMEM((3, n, rows, tokens), F32),
        pltpu.VMEM((3, n, rows, tokens), F32),
        pltpu.VMEM((2 * top, tokens), BF16),
        pltpu.VMEM((2, ff, half), BF16),
        pltpu.VMEM((2, ff, half), BF16),
        *[pltpu.VMEM((2, half, ff), BF16) for _ in range(4)],
        pltpu.VMEM((p.most * CAP, 2, ff), BF16),
        pltpu.VMEM((p.most * CAP, 2, ff), BF16),
        *[pltpu.VMEM((2, p.most * CAP, ff), F32) for _ in range(3)],
        *[pltpu.VMEM((2, p.most * CAP, 2 * ff + 128), BF16) for _ in range(2)],
        pltpu.VMEM((blocks, 1, 128), F32),
        pltpu.VMEM((n, planes, 1, 128), F32),
        dma((3,)), dma((3,)), dma((3,)), dma((3, n - 1, 2)), dma((3, n - 1, 2)),
        dma((3, nt, n)), dma((3, blocks)), dma((2,)), dma((2,)), dma((2,)), dma((2,)),
        dma((3, nt, n // 2 + 1)), dma((3, n)), dma((3, n - 1, 2)), dma((3, n - 1, 2)), dma((2,)),
        dma((1,)), dma((n,)), pltpu.SemaphoreType.REGULAR,
    ]
    grad_tokens, grad_combine = pl.pallas_call(
        functools.partial(kernel, p),
        out_shape=(
            jax.ShapeDtypeStruct((tokens, half), BF16),
            jax.ShapeDtypeStruct((top, tokens), BF16),
        ),
        in_specs=[vmem, vmem, vmem, hbm, hbm, hbm, hbm, hbm],
        out_specs=(vmem, vmem),
        scratch_shapes=scratch,
        compiler_params=pltpu.CompilerParams(
            collective_id=0, has_side_effects=True, vmem_limit_bytes=67043328
        ),
    )(expert_ids.T, combine.T, grad_out, saved_gate, saved_up, gate_weight, up_weight, down_weight)
    return grad_tokens, grad_combine.T


def solution(mesh, tiles=(27, 19, 18), step=256):
    n = round(mesh.shape["expert"] ** (1 / 3))

    def run(grad_out, combine, expert_ids, saved_gate, saved_up, gate_weight, up_weight, down_weight):
        plan = Plan(n, grad_out.shape[1], gate_weight.shape[2], expert_ids.shape[1], tiles, step)
        return on_device(
            plan, grad_out, combine, expert_ids, saved_gate, saved_up, gate_weight, up_weight, down_weight
        )

    in_specs = (
        P("expert", "etp"),
        P("expert", None),
        P("expert", None),
        P(None, "expert", "etp"),
        P(None, "expert", "etp"),
        P("expert", None, "etp"),
        P("expert", None, "etp"),
        P("expert", "etp", None),
    )
    out_specs = (P("expert", "etp"), P("expert", None))
    return jax.shard_map(run, mesh=mesh, in_specs=in_specs, out_specs=out_specs, check_vma=False)
```

```python
import functools
import itertools

import jax
import jax.numpy as jnp
from jax import lax
from jax.experimental import pallas as pl
from jax.experimental.pallas import tpu as pltpu
from jax.sharding import PartitionSpec as P

MESH = pl.DeviceIdType.MESH
BF16, F32, I32 = jnp.bfloat16, jnp.float32, jnp.int32
NT = (((1,), (1,)), ((), ()))
TN = (((0,), (0,)), ((), ()))
CAP = 16
AXES = ((0, 1, 2), (1, 2, 0), (2, 0, 1))


class Plan:
    def __init__(self, n, half, ff, top, tiles, step):
        self.n, self.half, self.ff, self.top, self.step = n, half, ff, top, step
        self.part = (half + 128) // 3
        self.base = (0, self.part, 2 * self.part - 128)
        far = lambda d: tuple(min(v, n - v) for v in d)
        self.order = sorted(itertools.product(range(n), repeat=3), key=lambda d: (max(far(d)), sum(d) % 2, d))
        self.slot = {d: i for i, d in enumerate(self.order)}
        self.tiles, start = [], 0
        for count in tiles:
            self.tiles.append((start, count))
            start += count
        self.most = max(tiles)
        self.tile = [t for t, count in enumerate(tiles) for _ in range(count)]
        self.offsets = sorted(range(1, n), key=lambda o: min(o, n - o))
        self.planes = n * n
        self.kind, load = {}, [0, 0, 0]
        for d in sorted(self.order, key=lambda d: -sum(far(d))):
            choices = []
            for kind in range(2):
                new = list(load)
                for f in range(3):
                    lo, hi = self.span_of(f, kind)
                    for axis in AXES[f][1:]:
                        new[axis] += (hi - lo) * far(d)[axis]
                choices.append((max(new), kind, new))
            _, self.kind[d], load = min(choices)
        self.peers = [d for d in self.order if 0 < sum(v > 0 for v in d) < 3]

    def span_of(self, f, kind):
        lo, hi = self.base[f], self.base[f] + self.part
        return (lo + 128 if (f, kind) == (2, 0) else lo, hi - 128 if (f, kind) == (1, 1) else hi)

    def span(self, f, d):
        return self.span_of(f, self.kind[d])

    def along(self, f, values):
        out = [0, 0, 0]
        for axis, value in zip(AXES[f], values):
            out[axis] = value
        return tuple(out)

    def seen(self, f, d):
        return tuple(d[axis] for axis in AXES[f])


def kernel(p, ids_ref, cw_ref, go_ref, sg_ref, su_ref, gw_ref, uw_ref, dn_ref, gt_ref, gc_ref,
           xo, s0, s1, s2, r0, r1, r2, g0, g1, g2, gm, ts, tr, gcs, gcr, codes, cws, meta,
           dna, dnb, gwa, gwb, uwa, uwb, sgt, sut, gbuf, pout, pin, hout, hin, dws, dwr,
           wsem, wss, wsr, s1s, s1r, ds, dr, ps, pr, hs, hr, rs, rr, tss, trs, sas, es, er, pace):
    n, half, part, planes = p.n, p.half, p.part, p.planes
    send, back, gath = (s0, s1, s2), (r0, r1, r2), (g0, g1, g2)
    me, core = lax.axis_index("expert"), lax.axis_index("etp")
    at = (me // (n * n), lax.rem(me // n, n), lax.rem(me, n))
    stride = (n * n, n, 1)

    def device(d, sign=1):
        c = [lax.rem(v + (sign * o) % n, n) for v, o in zip(at, d)]
        return (c[0] * stride[0] + c[1] * stride[1] + c[2], core)

    partner = (me, 1 - core)

    def block_of(d):
        return device(d, -1)[0]

    for f in (1, 2):
        for a in range(n):
            for q in range(planes):
                kind = p.kind[p.along(f, (a, q // n, q % n))]
                if f == 1 and kind == 1:
                    back[f][a, q, :, :, part - 128:part] = jnp.zeros((2, CAP, 128), BF16)
                if f == 2 and kind == 0:
                    back[f][a, q, :, :, 0:128] = jnp.zeros((2, CAP, 128), BF16)

    barrier = pltpu.get_barrier_semaphore()
    for d in p.peers:
        pl.semaphore_signal(barrier, inc=1, device_id=device(d), device_id_type=MESH)
    pl.semaphore_signal(barrier, inc=1, device_id=partner, device_id_type=MESH)

    def amount(size, sem):
        for lanes in (512, 256, 128):
            rows_in = size // (2 * lanes)
            if lanes <= p.ff and rows_in * 2 * lanes == size and rows_in % CAP == 0:
                break
        rows_at = gwa.at[0, pl.ds(0, rows_in), pl.ds(0, lanes)]
        return pltpu.make_async_remote_copy(
            src_ref=rows_at, dst_ref=rows_at, send_sem=sem, recv_sem=sem,
            device_id=partner, device_id_type=MESH)

    def bytes_of(spans, sem):
        return amount(sum(hi - lo for lo, hi in spans) * 4 * CAP, sem)

    def drain_sent(spans, sem):
        if spans:
            bytes_of(spans, sem).wait_send()

    own = pl.multiple_of(core * half, 128)
    other = pl.multiple_of((1 - core) * half, 128)
    loads = [
        pltpu.make_async_copy(dn_ref.at[:, :, pl.ds(own, half)], dna, wsem.at[0]),
        pltpu.make_async_copy(gw_ref.at[:, pl.ds(own, half), :], gwa, wsem.at[1]),
        pltpu.make_async_copy(uw_ref.at[:, pl.ds(own, half), :], uwa, wsem.at[2]),
    ]
    for load in loads:
        load.start()
    trades = [
        pltpu.make_async_remote_copy(
            src_ref=src, dst_ref=dst, send_sem=wss.at[i], recv_sem=wsr.at[i],
            device_id=partner, device_id_type=MESH)
        for i, (src, dst) in enumerate((
            (dn_ref.at[:, :, pl.ds(other, half)], dnb),
            (gw_ref.at[:, pl.ds(other, half), :], gwb),
            (uw_ref.at[:, pl.ds(other, half), :], uwb),
        ))
    ]

    def saved_start(t):
        first, count = p.tiles[t]
        for j in range(count):
            b = block_of(p.order[first + j])
            block = pl.ds(pl.multiple_of(b * CAP, CAP), CAP)
            rows_at = pl.ds(j * CAP, CAP)
            pltpu.make_async_copy(sg_ref.at[block], sgt.at[rows_at], sas.at[0]).start()
            pltpu.make_async_copy(su_ref.at[block], sut.at[rows_at], sas.at[1]).start()

    def saved_wait(t):
        count = p.tiles[t][1] * CAP
        pltpu.make_async_copy(sg_ref.at[pl.ds(0, count)], sgt.at[pl.ds(0, count)], sas.at[0]).wait()
        pltpu.make_async_copy(su_ref.at[pl.ds(0, count)], sut.at[pl.ds(0, count)], sas.at[1]).wait()

    saved_start(0)

    meta[...] = jnp.concatenate(
        [ids_ref[...].astype(F32), cw_ref[...].astype(F32)], axis=0
    ).astype(BF16)
    tokens = meta.shape[1]
    before = (
        lax.broadcasted_iota(I32, (tokens, tokens), 0)
        < lax.broadcasted_iota(I32, (tokens, tokens), 1)
    ).astype(F32).astype(BF16)
    rows = 2 * planes
    r_iota = lax.broadcasted_iota(I32, (rows, tokens), 0)

    def experts_of(f, place, which):
        a, b, c = AXES[f]
        vb = lax.rem(at[b] + place // n, n)
        vc = lax.rem(at[c] + lax.rem(place, n), n)
        return 2 * (at[a] * stride[a] + vb * stride[b] + vc * stride[c]) + which

    experts = [experts_of(f, r_iota // 2, lax.rem(r_iota, 2)).astype(F32) for f in range(3)]
    c_iota = lax.broadcasted_iota(I32, (rows, CAP, tokens), 1).astype(F32)

    def select(f, a, info, token_cols):
        info = info.astype(F32)
        match = jnp.zeros((rows, tokens), F32)
        weight = jnp.zeros((rows, tokens), F32)
        for k in range(p.top):
            hit = experts[f] == info[k:k + 1, :]
            match = jnp.where(hit, 1.0, match)
            weight = jnp.where(hit, info[p.top + k:p.top + k + 1, :], weight)
        position = jnp.dot(match.astype(BF16), before, preferred_element_type=F32)
        code = jnp.where(match > 0, position, -1.0)
        codes[f, a] = code
        cws[f, a] = weight
        hot = jnp.where(code[:, None, :] == c_iota, 1.0, 0.0)
        hot = hot.reshape(rows * CAP, tokens).astype(BF16)
        own_place = p.along(f, (a, 0, 0))
        own_slot, own_span = p.slot[own_place], p.span(f, own_place)
        for lo in range(0, part, 256):
            hi = min(lo + 256, part)
            picked = jnp.dot(hot, token_cols(lo, hi), preferred_element_type=F32).astype(BF16)
            picked = picked.reshape(planes, 2, CAP, hi - lo)
            send[f][a, :, :, :, lo:hi] = picked
            x_lo, x_hi = max(p.base[f] + lo, own_span[0]), min(p.base[f] + hi, own_span[1])
            if x_lo < x_hi:
                at_col = x_lo - p.base[f] - lo
                xo[own_slot, :, :, x_lo:x_hi] = picked[0, :, :, at_col:at_col + x_hi - x_lo]

    def dispatch_copy(f, a, q):
        b, c = q // n, q % n
        place = p.along(f, (a, b, c))
        slot, (lo, hi) = p.slot[place], p.span(f, place)
        return pltpu.make_async_remote_copy(
            src_ref=send[f].at[a, q, :, :, pl.ds(lo - p.base[f], hi - lo)],
            dst_ref=xo.at[slot, :, :, pl.ds(lo, hi - lo)],
            send_sem=ds.at[f, p.tile[slot], a],
            recv_sem=dr.at[f, p.tile[slot], a],
            device_id=device(p.along(f, (0, b, c))),
            device_id_type=MESH,
        )

    summed = [2 * tokens * part] * 2 + [2 * tokens * part + 4 * p.top * tokens]
    gathered = 2 * tokens * part + 4 * p.top * tokens

    def gather_copies(f, o):
        to = device(p.along(f, (o, 0, 0)))
        return (
            pltpu.make_async_remote_copy(
                src_ref=go_ref.at[:, pl.ds(p.base[f], part)],
                dst_ref=gath[f].at[o - 1],
                send_sem=s1s.at[f, o - 1], recv_sem=s1r.at[f, o - 1],
                device_id=to, device_id_type=MESH),
            pltpu.make_async_remote_copy(
                src_ref=meta, dst_ref=gm.at[f, o - 1],
                send_sem=s1s.at[f, o - 1], recv_sem=s1r.at[f, o - 1],
                device_id=to, device_id_type=MESH),
        )

    def dispatch(f, a, t):
        return [q for q in range(1, planes)
                if p.tile[p.slot[p.along(f, (a, q // n, q % n))]] == t]

    def dispatch_start(f, a, t):
        for q in dispatch(f, a, t):
            dispatch_copy(f, a, q).start()

    def dispatch_spans(f, a, t):
        return [p.span(f, p.along(f, (a, q // n, q % n))) for q in dispatch(f, a, t)]

    def dispatch_sent(f, a, t):
        drain_sent(dispatch_spans(f, a, t), ds.at[f, t, a])

    def group(a):
        return min(a, n - a)

    def returns(f, t, g):
        first, count = p.tiles[t]
        found = [(slot, p.seen(f, p.order[slot])) for slot in range(first, first + count)]
        return [(slot, d) for slot, d in found if group(d[0]) == g]

    def return_copy(f, t, slot):
        a, b, c = p.seen(f, p.order[slot])
        lo, hi = p.span(f, p.order[slot])
        return pltpu.make_async_remote_copy(
            src_ref=xo.at[slot, :, :, pl.ds(lo, hi - lo)],
            dst_ref=back[f].at[a, b * n + c, :, :, pl.ds(lo - p.base[f], hi - lo)],
            send_sem=rs.at[f, t, group(a)], recv_sem=rr.at[f, a],
            device_id=device(p.along(f, (0, b, c)), -1), device_id_type=MESH)

    def weight_copy(slot):
        a, b, c = p.seen(2, p.order[slot])
        return pltpu.make_async_remote_copy(
            src_ref=dws.at[slot], dst_ref=dwr.at[a, b * n + c], send_sem=es.at[0], recv_sem=er.at[a],
            device_id=device(p.along(2, (0, b, c)), -1), device_id_type=MESH)

    def return_start(t, g):
        lists = [returns(f, t, g) for f in range(3)]
        for i in range(max(len(v) for v in lists)):
            for f in range(3):
                if i < len(lists[f]):
                    slot, (a, b, c) = lists[f][i]
                    if (b, c) == (0, 0):
                        lo, hi = p.span(f, p.order[slot])
                        back[f][a, 0, :, :, lo - p.base[f]:hi - p.base[f]] = xo[slot, :, :, lo:hi]
                        if f == 2:
                            dwr[a, 0] = dws[slot]
                    else:
                        if f == 2:
                            weight_copy(slot).start()
                        return_copy(f, t, slot).start()

    def return_sent(t, g):
        for f in range(3):
            drain_sent([p.span(f, p.order[slot]) for slot, d in returns(f, t, g) if d[1:] != (0, 0)],
                       rs.at[f, t, g])

    last = len(p.tiles) - 1
    for f in range(3):
        select(f, 0, meta[...], lambda lo, hi: go_ref[:, p.base[f] + lo:p.base[f] + hi])
    pl.semaphore_wait(barrier, len(p.peers) + 1)
    for o in p.offsets:
        for f in range(3):
            for copy in gather_copies(f, o):
                copy.start()
    trades[0].start()
    for f in range(3):
        dispatch_start(f, 0, 0)
    for a in p.offsets:
        for f in range(3):
            amount(gathered, s1r.at[f, a - 1]).wait_recv()
            select(f, a, gm[f, a - 1], lambda lo, hi: gath[f][a - 1, :, lo:hi])
            dispatch_start(f, a, 0)
    for a in [0] + p.offsets:
        for f in range(3):
            dispatch_sent(f, a, 0)
    pl.semaphore_signal(pace, inc=1, device_id=partner, device_id_type=MESH)
    pl.semaphore_wait(pace, 1)
    if last >= 1:
        for a in [0] + p.offsets:
            for f in range(3):
                dispatch_start(f, a, 1)
    for trade in trades[1:]:
        trade.start()
    for t, (first, count) in enumerate(p.tiles):
        m = count * CAP
        for f in range(3):
            for a in range(n):
                spans = dispatch_spans(f, a, t)
                if spans:
                    bytes_of(spans, dr.at[f, t, a]).wait_recv()
        if t == 0:
            loads[0].wait()
            trades[0].wait_recv()

        def part_copy(l):
            return pltpu.make_async_remote_copy(
                src_ref=pout.at[l, pl.ds(0, m)], dst_ref=pin.at[l, pl.ds(0, m)],
                send_sem=ps.at[l], recv_sem=pr.at[l], device_id=partner, device_id_type=MESH)

        def hidden_copy(l):
            return pltpu.make_async_remote_copy(
                src_ref=hout.at[l, pl.ds(0, m)], dst_ref=hin.at[l, pl.ds(0, m)],
                send_sem=hs.at[l], recv_sem=hr.at[l], device_id=partner, device_id_type=MESH)

        def features(l):
            return xo[pl.ds(first, count), l, :, 0:half].reshape(m, half)

        def part_of_other(l, _):
            pout[l, 0:m, :] = lax.dot_general(features(l), dnb[l], NT, preferred_element_type=F32)
            part_copy(l).start()
            return 0

        def part_of_own(l, _):
            gbuf[l, 0:m, :] = lax.dot_general(features(l), dna[l], NT, preferred_element_type=F32)
            return 0

        def pointwise(l, j):
            at_row = pl.ds(pl.multiple_of(j * CAP, CAP), CAP)
            grad = gbuf[l, at_row, :] + pin[l, at_row, :]
            gate = jnp.swapaxes(sgt[at_row], 0, 1)[l].astype(F32)
            up = jnp.swapaxes(sut[at_row], 0, 1)[l].astype(F32)
            sig = 0.5 * jnp.tanh(0.5 * gate) + 0.5
            act = gate * sig
            gup = grad * act
            total = jnp.sum(gup * up, axis=1, keepdims=True)
            hout[l, at_row, 0:p.ff] = (grad * up * sig * (1.0 + gate * (1.0 - sig))).astype(BF16)
            hout[l, at_row, p.ff:2 * p.ff] = gup.astype(BF16)
            hout[l, at_row, 2 * p.ff:] = jnp.broadcast_to(total, (CAP, 128)).astype(BF16)

        def hidden():
            for l in range(2):
                part_copy(l).wait_recv()

                def two(i, _):
                    pointwise(l, 2 * i)
                    pointwise(l, 2 * i + 1)
                    return 0

                lax.fori_loop(0, count // 2, two, 0)
                if count % 2:
                    pointwise(l, count - 1)
                hidden_copy(l).start()

        def project(l, _):
            hidden_copy(l).wait_recv()
            for lo in range(0, half, p.step):
                u = None
                for h, gate_w, up_w in ((hout, gwa, uwa), (hin, gwb, uwb)):
                    for at_col, w in ((0, gate_w), (p.ff, up_w)):
                        term = lax.dot_general(
                            h[l, 0:m, at_col:at_col + p.ff], w[l, lo:lo + p.step, :], NT,
                            preferred_element_type=F32)
                        u = term if u is None else u + term
                xo[pl.ds(first, count), l, :, lo:lo + p.step] = u.astype(BF16).reshape(count, CAP, p.step)
            return 0

        def sent(copy):
            def wait(l, _):
                copy(l).wait_send()
                return 0
            lax.fori_loop(0, 2, wait, 0)

        lax.fori_loop(0, 2, part_of_other, 0)
        lax.fori_loop(0, 2, part_of_own, 0)
        saved_wait(t)
        hidden()
        if t < last:
            saved_start(t + 1)
        if t == 0:
            for load in loads[1:]:
                load.wait()
            for trade in trades[1:]:
                trade.wait_recv()
        if 0 < t + 2 <= last:
            for a in [0] + p.offsets:
                for f in range(3):
                    dispatch_start(f, a, t + 2)
        lax.fori_loop(0, 2, project, 0)
        row = None
        for l in range(2):
            sums = hout[l, 0:m, 2 * p.ff:].astype(F32) + hin[l, 0:m, 2 * p.ff:].astype(F32)
            sums = sums.astype(BF16).astype(F32).reshape(count, CAP, 128)
            shape = (count, CAP, 128)
            lane = lax.rem(lax.broadcasted_iota(I32, shape, 2), 2 * CAP)
            mine = lane == l * CAP + lax.broadcasted_iota(I32, shape, 1)
            term = jnp.sum(jnp.where(mine, sums, 0.0), axis=1, keepdims=True)
            row = term if row is None else row + term
        dws[pl.ds(first, count)] = row
        sent(part_copy)
        sent(hidden_copy)
        for g in range(n // 2, 0, -1):
            return_start(t, g)

    def total_copy(f, o):
        to = device(p.along(f, (o, 0, 0)), -1)
        copies = [pltpu.make_async_remote_copy(
            src_ref=ts.at[f, o - 1], dst_ref=tr.at[f, o - 1],
            send_sem=tss.at[f, o - 1], recv_sem=trs.at[f, o - 1],
            device_id=to, device_id_type=MESH)]
        if f == 2:
            copies.append(pltpu.make_async_remote_copy(
                src_ref=gcs.at[o - 1], dst_ref=gcr.at[o - 1],
                send_sem=tss.at[f, o - 1], recv_sem=trs.at[f, o - 1],
                device_id=to, device_id_type=MESH))
        return copies

    def back_wait(f, a):
        spans = [p.span(f, p.along(f, (a, q // n, q % n))) for q in range(1, planes)]
        bytes_of(spans, rr.at[f, a]).wait_recv()
        if f == 2:
            pltpu.make_async_remote_copy(
                src_ref=dwr.at[a, pl.ds(1, planes - 1)], dst_ref=dwr.at[a, pl.ds(1, planes - 1)],
                send_sem=es.at[0], recv_sem=er.at[a],
                device_id=partner, device_id_type=MESH).wait_recv()

    def combined(f, a, info):
        back_wait(f, a)
        hit = codes[f, a][:, None, :] == c_iota
        weight = jnp.where(hit, cws[f, a][:, None, :], 0.0)
        weight = weight.reshape(rows * CAP, tokens).astype(BF16)
        values = back[f][a].reshape(rows * CAP, part)
        total = lax.dot_general(weight, values, TN, preferred_element_type=F32)
        if f < 2:
            return total, None
        hot = jnp.where(hit, 1.0, 0.0).reshape(rows * CAP, tokens).astype(BF16)
        values = dwr[a].reshape(planes, 128)
        wide = jnp.concatenate([values] * (rows * CAP // 128), axis=1)
        wide = jnp.concatenate([wide, wide], axis=0)
        lane = lax.broadcasted_iota(I32, wide.shape, 1)
        line = lax.broadcasted_iota(I32, wide.shape, 0)
        mine = lane // CAP == 2 * lax.rem(line, planes) + line // planes
        wide = jnp.where(mine, wide, 0.0).astype(BF16)
        spread = jnp.dot(wide, hot, preferred_element_type=F32)
        info = info.astype(F32)
        by_choice = experts_of(f, lax.rem(r_iota, planes), r_iota // planes).astype(F32)
        picked = [
            jnp.sum(jnp.where(by_choice == info[k:k + 1, :], spread, 0.0), axis=0, keepdims=True)
            for k in range(p.top)
        ]
        return total, jnp.concatenate(picked, axis=0)

    def partial_sums(a):
        for f in range(3):
            total, sums = combined(f, a, gm[f, a - 1])
            ts[f, a - 1] = total.astype(BF16)
            if f == 2:
                gcs[a - 1] = sums
            for copy in total_copy(f, a):
                copy.start()

    for t in range(last):
        for g in range(1, n // 2 + 1):
            return_sent(t, g)
    if n > 2:
        return_sent(last, n // 2)
    return_start(0, 0)
    for a in p.offsets[::-1]:
        if group(a) == 1 and a == p.offsets[::-1][0 if n == 2 else 1]:
            return_sent(last, 1)
            for t in range(1, last + 1):
                return_start(t, 0)
        partial_sums(a)
    shared = None
    for f in range(3):
        total, sums = combined(f, 0, meta[...])
        for a in range(1, n):
            amount(summed[f], trs.at[f, a - 1]).wait_recv()
            total = total + tr[f, a - 1].astype(F32)
            if f == 2:
                sums = sums + gcr[a - 1]
        lo, hi = 0, part
        if f == 1:
            shared, hi = total[:, part - 128:], part - 128
        if f == 2:
            gt_ref[:, p.base[2]:p.base[2] + 128] = (total[:, 0:128] + shared).astype(BF16)
            gc_ref[...] = sums.astype(BF16)
            lo = 128
        gt_ref[:, p.base[f] + lo:p.base[f] + hi] = total[:, lo:hi].astype(BF16)

    for f in range(3):
        for o in range(1, n):
            amount(gathered, s1s.at[f, o - 1]).wait_send()
            amount(summed[f], tss.at[f, o - 1]).wait_send()
        for t in range(1, last + 1):
            for a in range(n):
                dispatch_sent(f, a, t)
    for t in range(last + 1):
        for g in range(n // 2 + 1):
            if g == 0:
                return_sent(t, g)
    sent_rows = sum(p.seen(2, d)[1:] != (0, 0) for d in p.order)
    pltpu.make_async_remote_copy(
        src_ref=dws.at[pl.ds(0, sent_rows)], dst_ref=dws.at[pl.ds(0, sent_rows)],
        send_sem=es.at[0], recv_sem=er.at[0], device_id=partner, device_id_type=MESH).wait_send()
    for trade in trades:
        trade.wait_send()


def on_device(plan, grad_out, combine, expert_ids, saved_gate, saved_up, gate_weight, up_weight, down_weight):
    p = plan
    n, half, ff, part, planes = p.n, p.half, p.ff, p.part, p.planes
    tokens, top = expert_ids.shape
    blocks, nt = n * n * n, len(p.tiles)
    vmem = pl.BlockSpec(memory_space=pltpu.VMEM)
    hbm = pl.BlockSpec(memory_space=pl.ANY)
    dma = pltpu.SemaphoreType.DMA
    rows = 2 * planes
    scratch = [
        pltpu.VMEM((blocks, 2, CAP, half), BF16),
        *[pltpu.VMEM((n, planes, 2, CAP, part), BF16) for _ in range(6)],
        *[pltpu.VMEM((n - 1, tokens, part), BF16) for _ in range(3)],
        pltpu.VMEM((3, n - 1, 2 * top, tokens), BF16),
        pltpu.VMEM((3, n - 1, tokens, part), BF16),
        pltpu.VMEM((3, n - 1, tokens, part), BF16),
        pltpu.VMEM((n - 1, top, tokens), F32),
        pltpu.VMEM((n - 1, top, tokens), F32),
        pltpu.VMEM((3, n, rows, tokens), F32),
        pltpu.VMEM((3, n, rows, tokens), F32),
        pltpu.VMEM((2 * top, tokens), BF16),
        pltpu.VMEM((2, ff, half), BF16),
        pltpu.VMEM((2, ff, half), BF16),
        *[pltpu.VMEM((2, half, ff), BF16) for _ in range(4)],
        pltpu.VMEM((p.most * CAP, 2, ff), BF16),
        pltpu.VMEM((p.most * CAP, 2, ff), BF16),
        *[pltpu.VMEM((2, p.most * CAP, ff), F32) for _ in range(3)],
        *[pltpu.VMEM((2, p.most * CAP, 2 * ff + 128), BF16) for _ in range(2)],
        pltpu.VMEM((blocks, 1, 128), F32),
        pltpu.VMEM((n, planes, 1, 128), F32),
        dma((3,)), dma((3,)), dma((3,)), dma((3, n - 1)), dma((3, n - 1)),
        dma((3, nt, n)), dma((3, nt, n)), dma((2,)), dma((2,)), dma((2,)), dma((2,)),
        dma((3, nt, n // 2 + 1)), dma((3, n)), dma((3, n - 1)), dma((3, n - 1)), dma((2,)),
        dma((1,)), dma((n,)), pltpu.SemaphoreType.REGULAR,
    ]
    grad_tokens, grad_combine = pl.pallas_call(
        functools.partial(kernel, p),
        out_shape=(
            jax.ShapeDtypeStruct((tokens, half), BF16),
            jax.ShapeDtypeStruct((top, tokens), BF16),
        ),
        in_specs=[vmem, vmem, vmem, hbm, hbm, hbm, hbm, hbm],
        out_specs=(vmem, vmem),
        scratch_shapes=scratch,
        compiler_params=pltpu.CompilerParams(
            collective_id=0, has_side_effects=True, vmem_limit_bytes=67043328
        ),
    )(expert_ids.T, combine.T, grad_out, saved_gate, saved_up, gate_weight, up_weight, down_weight)
    return grad_tokens, grad_combine.T


def solution(mesh, tiles=(27, 19, 18), step=256):
    n = round(mesh.shape["expert"] ** (1 / 3))

    def run(grad_out, combine, expert_ids, saved_gate, saved_up, gate_weight, up_weight, down_weight):
        plan = Plan(n, grad_out.shape[1], gate_weight.shape[2], expert_ids.shape[1], tiles, step)
        return on_device(
            plan, grad_out, combine, expert_ids, saved_gate, saved_up, gate_weight, up_weight, down_weight
        )

    in_specs = (
        P("expert", "etp"),
        P("expert", None),
        P("expert", None),
        P(None, "expert", "etp"),
        P(None, "expert", "etp"),
        P("expert", None, "etp"),
        P("expert", None, "etp"),
        P("expert", "etp", None),
    )
    out_specs = (P("expert", "etp"), P("expert", None))
    return jax.shard_map(run, mesh=mesh, in_specs=in_specs, out_specs=out_specs, check_vma=False)
```

```python
import functools
import itertools

import jax
import jax.numpy as jnp
from jax import lax
from jax.experimental import pallas as pl
from jax.experimental.pallas import tpu as pltpu
from jax.sharding import PartitionSpec as P

MESH = pl.DeviceIdType.MESH
BF16, F32, I32 = jnp.bfloat16, jnp.float32, jnp.int32
NT = (((1,), (1,)), ((), ()))
TN = (((0,), (0,)), ((), ()))
CAP = 16
AXES = ((0, 1, 2), (1, 2, 0), (2, 0, 1))


class Plan:
    def __init__(self, n, half, ff, top, tiles, step):
        self.n, self.half, self.ff, self.top, self.step = n, half, ff, top, step
        self.part = (half + 128) // 3
        self.base = (0, self.part, 2 * self.part - 128)
        far = lambda d: tuple(min(v, n - v) for v in d)
        self.order = sorted(itertools.product(range(n), repeat=3), key=lambda d: (max(far(d)), sum(d) % 2, d))
        self.slot = {d: i for i, d in enumerate(self.order)}
        self.tiles, start = [], 0
        for count in tiles:
            self.tiles.append((start, count))
            start += count
        self.most = max(tiles)
        self.tile = [t for t, count in enumerate(tiles) for _ in range(count)]
        self.offsets = sorted(range(1, n), key=lambda o: min(o, n - o))
        self.planes = n * n
        self.kind, load = {}, [0, 0, 0]
        for d in sorted(self.order, key=lambda d: -sum(far(d))):
            choices = []
            for kind in range(2):
                new = list(load)
                for f in range(3):
                    lo, hi = self.span_of(f, kind)
                    for axis in AXES[f][1:]:
                        new[axis] += (hi - lo) * far(d)[axis]
                choices.append((max(new), kind, new))
            _, self.kind[d], load = min(choices)
        self.peers = [d for d in self.order if 0 < sum(v > 0 for v in d) < 3]

    def span_of(self, f, kind):
        lo, hi = self.base[f], self.base[f] + self.part
        return (lo + 128 if (f, kind) == (2, 0) else lo, hi - 128 if (f, kind) == (1, 1) else hi)

    def span(self, f, d):
        return self.span_of(f, self.kind[d])

    def along(self, f, values):
        out = [0, 0, 0]
        for axis, value in zip(AXES[f], values):
            out[axis] = value
        return tuple(out)

    def seen(self, f, d):
        return tuple(d[axis] for axis in AXES[f])


def kernel(p, ids_ref, cw_ref, go_ref, sg_ref, su_ref, gw_ref, uw_ref, dn_ref, gt_ref, gc_ref,
           xo, s0, s1, s2, r0, r1, r2, g0, g1, g2, gm, ts, tr, gcs, gcr, codes, cws, meta,
           dna, dnb, gwa, gwb, uwa, uwb, sgt, sut, gbuf, pout, pin, hout, hin, dws, dwr,
           wsem, wss, wsr, s1s, s1r, ds, dr, ps, pr, hs, hr, rs, rr, tss, trs, sas, es, er, pace):
    n, half, part, planes = p.n, p.half, p.part, p.planes
    send, back, gath = (s0, s1, s2), (r0, r1, r2), (g0, g1, g2)
    me, core = lax.axis_index("expert"), lax.axis_index("etp")
    at = (me // (n * n), lax.rem(me // n, n), lax.rem(me, n))
    stride = (n * n, n, 1)

    def device(d, sign=1):
        c = [lax.rem(v + (sign * o) % n, n) for v, o in zip(at, d)]
        return (c[0] * stride[0] + c[1] * stride[1] + c[2], core)

    partner = (me, 1 - core)

    def block_of(d):
        return device(d, -1)[0]

    for f in (1, 2):
        for a in range(n):
            for q in range(planes):
                kind = p.kind[p.along(f, (a, q // n, q % n))]
                if f == 1 and kind == 1:
                    back[f][a, q, :, :, part - 128:part] = jnp.zeros((2, CAP, 128), BF16)
                if f == 2 and kind == 0:
                    back[f][a, q, :, :, 0:128] = jnp.zeros((2, CAP, 128), BF16)

    barrier = pltpu.get_barrier_semaphore()
    for d in p.peers:
        pl.semaphore_signal(barrier, inc=1, device_id=device(d), device_id_type=MESH)
    pl.semaphore_signal(barrier, inc=1, device_id=partner, device_id_type=MESH)

    def amount(size, sem):
        units = size // (2 * CAP * 128)
        found = [
            (blocks, lines, units // (lines * blocks))
            for lines in (2, 1) for blocks in range(1, xo.shape[0] + 1)
            if units % (lines * blocks) == 0 and units // (lines * blocks) <= half // 128
        ]
        if found and units * 2 * CAP * 128 == size:
            blocks, lines, wide = found[0]
            rows_at = xo.at[pl.ds(0, blocks), pl.ds(0, lines), :, pl.ds(0, 128 * wide)]
        else:
            lanes = 256 if size % (512 * CAP) == 0 and p.ff >= 256 else 128
            rows_at = gwa.at[0, pl.ds(0, size // (2 * lanes)), pl.ds(0, lanes)]
        return pltpu.make_async_remote_copy(
            src_ref=rows_at, dst_ref=rows_at, send_sem=sem, recv_sem=sem,
            device_id=partner, device_id_type=MESH)

    def bytes_of(spans, sem):
        return amount(sum(hi - lo for lo, hi in spans) * 4 * CAP, sem)

    def drain_sent(spans, sem):
        if spans:
            bytes_of(spans, sem).wait_send()

    own = pl.multiple_of(core * half, 128)
    other = pl.multiple_of((1 - core) * half, 128)
    loads = [
        pltpu.make_async_copy(dn_ref.at[:, :, pl.ds(own, half)], dna, wsem.at[0]),
        pltpu.make_async_copy(gw_ref.at[:, pl.ds(own, half), :], gwa, wsem.at[1]),
        pltpu.make_async_copy(uw_ref.at[:, pl.ds(own, half), :], uwa, wsem.at[2]),
    ]
    for load in loads:
        load.start()
    trades = [
        pltpu.make_async_remote_copy(
            src_ref=src, dst_ref=dst, send_sem=wss.at[i], recv_sem=wsr.at[i],
            device_id=partner, device_id_type=MESH)
        for i, (src, dst) in enumerate((
            (dn_ref.at[:, :, pl.ds(other, half)], dnb),
            (gw_ref.at[:, pl.ds(other, half), :], gwb),
            (uw_ref.at[:, pl.ds(other, half), :], uwb),
        ))
    ]

    def saved_start(t):
        first, count = p.tiles[t]
        for j in range(count):
            b = block_of(p.order[first + j])
            block = pl.ds(pl.multiple_of(b * CAP, CAP), CAP)
            rows_at = pl.ds(j * CAP, CAP)
            pltpu.make_async_copy(sg_ref.at[block], sgt.at[rows_at], sas.at[0]).start()
            pltpu.make_async_copy(su_ref.at[block], sut.at[rows_at], sas.at[1]).start()

    def saved_wait(t):
        count = p.tiles[t][1] * CAP
        pltpu.make_async_copy(sg_ref.at[pl.ds(0, count)], sgt.at[pl.ds(0, count)], sas.at[0]).wait()
        pltpu.make_async_copy(su_ref.at[pl.ds(0, count)], sut.at[pl.ds(0, count)], sas.at[1]).wait()

    saved_start(0)

    meta[...] = jnp.concatenate(
        [ids_ref[...].astype(F32), cw_ref[...].astype(F32)], axis=0
    ).astype(BF16)
    tokens = meta.shape[1]
    before = (
        lax.broadcasted_iota(I32, (tokens, tokens), 0)
        < lax.broadcasted_iota(I32, (tokens, tokens), 1)
    ).astype(F32).astype(BF16)
    rows = 2 * planes
    r_iota = lax.broadcasted_iota(I32, (rows, tokens), 0)

    def experts_of(f, place, which):
        a, b, c = AXES[f]
        vb = lax.rem(at[b] + place // n, n)
        vc = lax.rem(at[c] + lax.rem(place, n), n)
        return 2 * (at[a] * stride[a] + vb * stride[b] + vc * stride[c]) + which

    experts = [experts_of(f, r_iota // 2, lax.rem(r_iota, 2)).astype(F32) for f in range(3)]
    c_iota = lax.broadcasted_iota(I32, (rows, CAP, tokens), 1).astype(F32)

    def select(f, a, info, token_cols):
        info = info.astype(F32)
        match = jnp.zeros((rows, tokens), F32)
        weight = jnp.zeros((rows, tokens), F32)
        for k in range(p.top):
            hit = experts[f] == info[k:k + 1, :]
            match = jnp.where(hit, 1.0, match)
            weight = jnp.where(hit, info[p.top + k:p.top + k + 1, :], weight)
        position = jnp.dot(match.astype(BF16), before, preferred_element_type=F32)
        code = jnp.where(match > 0, position, -1.0)
        codes[f, a] = code
        cws[f, a] = weight
        hot = jnp.where(code[:, None, :] == c_iota, 1.0, 0.0)
        hot = hot.reshape(rows * CAP, tokens).astype(BF16)
        own_place = p.along(f, (a, 0, 0))
        own_slot, own_span = p.slot[own_place], p.span(f, own_place)
        for lo in range(0, part, 256):
            hi = min(lo + 256, part)
            picked = jnp.dot(hot, token_cols(lo, hi), preferred_element_type=F32).astype(BF16)
            picked = picked.reshape(planes, 2, CAP, hi - lo)
            send[f][a, :, :, :, lo:hi] = picked
            x_lo, x_hi = max(p.base[f] + lo, own_span[0]), min(p.base[f] + hi, own_span[1])
            if x_lo < x_hi:
                at_col = x_lo - p.base[f] - lo
                xo[own_slot, :, :, x_lo:x_hi] = picked[0, :, :, at_col:at_col + x_hi - x_lo]

    def dispatch_copy(f, a, q):
        b, c = q // n, q % n
        place = p.along(f, (a, b, c))
        slot, (lo, hi) = p.slot[place], p.span(f, place)
        return pltpu.make_async_remote_copy(
            src_ref=send[f].at[a, q, :, :, pl.ds(lo - p.base[f], hi - lo)],
            dst_ref=xo.at[slot, :, :, pl.ds(lo, hi - lo)],
            send_sem=ds.at[f, p.tile[slot]],
            recv_sem=dr.at[f, p.tile[slot]],
            device_id=device(p.along(f, (0, b, c))),
            device_id_type=MESH,
        )

    summed = [2 * tokens * part] * 2 + [2 * tokens * part + 4 * p.top * tokens]
    gathered = 2 * tokens * part + 4 * p.top * tokens

    def gather_copies(f, o):
        to = device(p.along(f, (o, 0, 0)))
        return (
            pltpu.make_async_remote_copy(
                src_ref=go_ref.at[:, pl.ds(p.base[f], part)],
                dst_ref=gath[f].at[o - 1],
                send_sem=s1s.at[f], recv_sem=s1r.at[f, o - 1],
                device_id=to, device_id_type=MESH),
            pltpu.make_async_remote_copy(
                src_ref=meta, dst_ref=gm.at[f, o - 1],
                send_sem=s1s.at[f], recv_sem=s1r.at[f, o - 1],
                device_id=to, device_id_type=MESH),
        )

    def dispatch(f, a, t):
        return [q for q in range(1, planes)
                if p.tile[p.slot[p.along(f, (a, q // n, q % n))]] == t]

    def dispatch_start(f, a, t):
        for q in dispatch(f, a, t):
            dispatch_copy(f, a, q).start()

    def dispatch_spans(f, a, t):
        return [p.span(f, p.along(f, (a, q // n, q % n))) for q in dispatch(f, a, t)]

    def tile_spans(f, t):
        return [span for a in range(n) for span in dispatch_spans(f, a, t)]

    def dispatch_sent(t):
        for f in range(3):
            drain_sent(tile_spans(f, t), ds.at[f, t])

    def group(a):
        return min(a, n - a)

    def returns(f, t, g):
        first, count = p.tiles[t]
        found = [(slot, p.seen(f, p.order[slot])) for slot in range(first, first + count)]
        return [(slot, d) for slot, d in found if group(d[0]) == g]

    def return_copy(f, t, slot):
        a, b, c = p.seen(f, p.order[slot])
        lo, hi = p.span(f, p.order[slot])
        return pltpu.make_async_remote_copy(
            src_ref=xo.at[slot, :, :, pl.ds(lo, hi - lo)],
            dst_ref=back[f].at[a, b * n + c, :, :, pl.ds(lo - p.base[f], hi - lo)],
            send_sem=rs.at[f, return_group(t, group(a))], recv_sem=rr.at[f, a],
            device_id=device(p.along(f, (0, b, c)), -1), device_id_type=MESH)

    def weight_copy(slot):
        a, b, c = p.seen(2, p.order[slot])
        return pltpu.make_async_remote_copy(
            src_ref=dws.at[slot], dst_ref=dwr.at[a, b * n + c], send_sem=es.at[0], recv_sem=er.at[a],
            device_id=device(p.along(2, (0, b, c)), -1), device_id_type=MESH)

    def return_start(t, g):
        lists = [returns(f, t, g) for f in range(3)]
        for i in range(max(len(v) for v in lists)):
            for f in range(3):
                if i < len(lists[f]):
                    slot, (a, b, c) = lists[f][i]
                    if (b, c) == (0, 0):
                        lo, hi = p.span(f, p.order[slot])
                        back[f][a, 0, :, :, lo - p.base[f]:hi - p.base[f]] = xo[slot, :, :, lo:hi]
                        if f == 2:
                            dwr[a, 0] = dws[slot]
                    else:
                        if f == 2:
                            weight_copy(slot).start()
                        return_copy(f, t, slot).start()

    def return_group(t, g):
        return 3 if g > 0 and t < len(p.tiles) - 1 else g

    def return_sent(which):
        for f in range(3):
            drain_sent(
                [p.span(f, p.order[slot]) for t in range(len(p.tiles)) for g in range(n // 2 + 1)
                 for slot, d in returns(f, t, g)
                 if return_group(t, g) == which and d[1:] != (0, 0)],
                rs.at[f, which])

    last = len(p.tiles) - 1
    for f in range(3):
        select(f, 0, meta[...], lambda lo, hi: go_ref[:, p.base[f] + lo:p.base[f] + hi])
    pl.semaphore_wait(barrier, len(p.peers) + 1)
    for o in p.offsets:
        for f in range(3):
            for copy in gather_copies(f, o):
                copy.start()
    trades[0].start()
    for f in range(3):
        dispatch_start(f, 0, 0)
    for a in p.offsets:
        for f in range(3):
            amount(gathered, s1r.at[f, a - 1]).wait_recv()
            select(f, a, gm[f, a - 1], lambda lo, hi: gath[f][a - 1, :, lo:hi])
            dispatch_start(f, a, 0)
    dispatch_sent(0)
    pl.semaphore_signal(pace, inc=1, device_id=partner, device_id_type=MESH)
    pl.semaphore_wait(pace, 1)
    if last >= 1:
        for a in [0] + p.offsets:
            for f in range(3):
                dispatch_start(f, a, 1)
    for trade in trades[1:]:
        trade.start()
    for t, (first, count) in enumerate(p.tiles):
        m = count * CAP
        for f in range(3):
            if tile_spans(f, t):
                bytes_of(tile_spans(f, t), dr.at[f, t]).wait_recv()
        if t == 0:
            loads[0].wait()
            trades[0].wait_recv()

        def part_copy(l):
            return pltpu.make_async_remote_copy(
                src_ref=pout.at[l, pl.ds(0, m)], dst_ref=pin.at[l, pl.ds(0, m)],
                send_sem=ps.at[l], recv_sem=pr.at[l], device_id=partner, device_id_type=MESH)

        def hidden_copy(l):
            return pltpu.make_async_remote_copy(
                src_ref=hout.at[l, pl.ds(0, m)], dst_ref=hin.at[l, pl.ds(0, m)],
                send_sem=hs.at[l], recv_sem=hr.at[l], device_id=partner, device_id_type=MESH)

        def features(l):
            return xo[pl.ds(first, count), l, :, 0:half].reshape(m, half)

        def part_of_other(l, _):
            pout[l, 0:m, :] = lax.dot_general(features(l), dnb[l], NT, preferred_element_type=F32)
            part_copy(l).start()
            return 0

        def part_of_own(l, _):
            gbuf[l, 0:m, :] = lax.dot_general(features(l), dna[l], NT, preferred_element_type=F32)
            return 0

        def pointwise(l, j):
            at_row = pl.ds(pl.multiple_of(j * CAP, CAP), CAP)
            grad = gbuf[l, at_row, :] + pin[l, at_row, :]
            gate = jnp.swapaxes(sgt[at_row], 0, 1)[l].astype(F32)
            up = jnp.swapaxes(sut[at_row], 0, 1)[l].astype(F32)
            sig = 0.5 * jnp.tanh(0.5 * gate) + 0.5
            act = gate * sig
            gup = grad * act
            total = jnp.sum(gup * up, axis=1, keepdims=True)
            hout[l, at_row, 0:p.ff] = (grad * up * sig * (1.0 + gate * (1.0 - sig))).astype(BF16)
            hout[l, at_row, p.ff:2 * p.ff] = gup.astype(BF16)
            hout[l, at_row, 2 * p.ff:] = jnp.broadcast_to(total, (CAP, 128)).astype(BF16)

        def hidden():
            for l in range(2):
                part_copy(l).wait_recv()

                def two(i, _):
                    pointwise(l, 2 * i)
                    pointwise(l, 2 * i + 1)
                    return 0

                lax.fori_loop(0, count // 2, two, 0)
                if count % 2:
                    pointwise(l, count - 1)
                hidden_copy(l).start()

        def project(l, _):
            hidden_copy(l).wait_recv()
            for lo in range(0, half, p.step):
                u = None
                for h, gate_w, up_w in ((hout, gwa, uwa), (hin, gwb, uwb)):
                    for at_col, w in ((0, gate_w), (p.ff, up_w)):
                        term = lax.dot_general(
                            h[l, 0:m, at_col:at_col + p.ff], w[l, lo:lo + p.step, :], NT,
                            preferred_element_type=F32)
                        u = term if u is None else u + term
                xo[pl.ds(first, count), l, :, lo:lo + p.step] = u.astype(BF16).reshape(count, CAP, p.step)
            return 0

        def sent(copy):
            def wait(l, _):
                copy(l).wait_send()
                return 0
            lax.fori_loop(0, 2, wait, 0)

        lax.fori_loop(0, 2, part_of_other, 0)
        lax.fori_loop(0, 2, part_of_own, 0)
        saved_wait(t)
        hidden()
        if t < last:
            saved_start(t + 1)
        if t == 0:
            for load in loads[1:]:
                load.wait()
            for trade in trades[1:]:
                trade.wait_recv()
        if 0 < t + 2 <= last:
            for a in [0] + p.offsets:
                for f in range(3):
                    dispatch_start(f, a, t + 2)
        lax.fori_loop(0, 2, project, 0)
        row = None
        for l in range(2):
            sums = hout[l, 0:m, 2 * p.ff:].astype(F32) + hin[l, 0:m, 2 * p.ff:].astype(F32)
            sums = sums.astype(BF16).astype(F32).reshape(count, CAP, 128)
            shape = (count, CAP, 128)
            lane = lax.rem(lax.broadcasted_iota(I32, shape, 2), 2 * CAP)
            mine = lane == l * CAP + lax.broadcasted_iota(I32, shape, 1)
            term = jnp.sum(jnp.where(mine, sums, 0.0), axis=1, keepdims=True)
            row = term if row is None else row + term
        dws[pl.ds(first, count)] = row
        sent(part_copy)
        sent(hidden_copy)
        for g in range(n // 2, 0, -1):
            return_start(t, g)

    def total_copy(f, o):
        to = device(p.along(f, (o, 0, 0)), -1)
        copies = [pltpu.make_async_remote_copy(
            src_ref=ts.at[f, o - 1], dst_ref=tr.at[f, o - 1],
            send_sem=tss.at[f], recv_sem=trs.at[f],
            device_id=to, device_id_type=MESH)]
        if f == 2:
            copies.append(pltpu.make_async_remote_copy(
                src_ref=gcs.at[o - 1], dst_ref=gcr.at[o - 1],
                send_sem=tss.at[f], recv_sem=trs.at[f],
                device_id=to, device_id_type=MESH))
        return copies

    def back_wait(f, a):
        spans = [p.span(f, p.along(f, (a, q // n, q % n))) for q in range(1, planes)]
        bytes_of(spans, rr.at[f, a]).wait_recv()
        if f == 2:
            pltpu.make_async_remote_copy(
                src_ref=dwr.at[a, pl.ds(1, planes - 1)], dst_ref=dwr.at[a, pl.ds(1, planes - 1)],
                send_sem=es.at[0], recv_sem=er.at[a],
                device_id=partner, device_id_type=MESH).wait_recv()

    def combined(f, a, info):
        back_wait(f, a)
        hit = codes[f, a][:, None, :] == c_iota
        weight = jnp.where(hit, cws[f, a][:, None, :], 0.0)
        weight = weight.reshape(rows * CAP, tokens).astype(BF16)
        values = back[f][a].reshape(rows * CAP, part)
        total = lax.dot_general(weight, values, TN, preferred_element_type=F32)
        if f < 2:
            return total, None
        hot = jnp.where(hit, 1.0, 0.0).reshape(rows * CAP, tokens).astype(BF16)
        values = dwr[a].reshape(planes, 128)
        wide = jnp.concatenate([values] * (rows * CAP // 128), axis=1)
        wide = jnp.concatenate([wide, wide], axis=0)
        lane = lax.broadcasted_iota(I32, wide.shape, 1)
        line = lax.broadcasted_iota(I32, wide.shape, 0)
        mine = lane // CAP == 2 * lax.rem(line, planes) + line // planes
        wide = jnp.where(mine, wide, 0.0).astype(BF16)
        spread = jnp.dot(wide, hot, preferred_element_type=F32)
        info = info.astype(F32)
        by_choice = experts_of(f, lax.rem(r_iota, planes), r_iota // planes).astype(F32)
        picked = [
            jnp.sum(jnp.where(by_choice == info[k:k + 1, :], spread, 0.0), axis=0, keepdims=True)
            for k in range(p.top)
        ]
        return total, jnp.concatenate(picked, axis=0)

    def partial_sums(a):
        for f in range(3):
            total, sums = combined(f, a, gm[f, a - 1])
            ts[f, a - 1] = total.astype(BF16)
            if f == 2:
                gcs[a - 1] = sums
            for copy in total_copy(f, a):
                copy.start()

    return_sent(3)
    if n > 2:
        return_sent(2)
    return_start(0, 0)
    for a in p.offsets[::-1]:
        if group(a) == 1 and a == p.offsets[::-1][0 if n == 2 else 1]:
            return_sent(1)
            for t in range(1, last + 1):
                return_start(t, 0)
        partial_sums(a)
    shared = None
    for f in range(3):
        total, sums = combined(f, 0, meta[...])
        amount((n - 1) * summed[f], trs.at[f]).wait_recv()
        for a in range(1, n):
            total = total + tr[f, a - 1].astype(F32)
            if f == 2:
                sums = sums + gcr[a - 1]
        lo, hi = 0, part
        if f == 1:
            shared, hi = total[:, part - 128:], part - 128
        if f == 2:
            gt_ref[:, p.base[2]:p.base[2] + 128] = (total[:, 0:128] + shared).astype(BF16)
            gc_ref[...] = sums.astype(BF16)
            lo = 128
        gt_ref[:, p.base[f] + lo:p.base[f] + hi] = total[:, lo:hi].astype(BF16)

    for f in range(3):
        amount((n - 1) * gathered, s1s.at[f]).wait_send()
        amount((n - 1) * summed[f], tss.at[f]).wait_send()
    for t in range(1, last + 1):
        dispatch_sent(t)
    return_sent(0)
    sent_rows = sum(p.seen(2, d)[1:] != (0, 0) for d in p.order)
    pltpu.make_async_remote_copy(
        src_ref=dws.at[pl.ds(0, sent_rows)], dst_ref=dws.at[pl.ds(0, sent_rows)],
        send_sem=es.at[0], recv_sem=er.at[0], device_id=partner, device_id_type=MESH).wait_send()
    for trade in trades:
        trade.wait_send()


def on_device(plan, grad_out, combine, expert_ids, saved_gate, saved_up, gate_weight, up_weight, down_weight):
    p = plan
    n, half, ff, part, planes = p.n, p.half, p.ff, p.part, p.planes
    tokens, top = expert_ids.shape
    blocks, nt = n * n * n, len(p.tiles)
    vmem = pl.BlockSpec(memory_space=pltpu.VMEM)
    hbm = pl.BlockSpec(memory_space=pl.ANY)
    dma = pltpu.SemaphoreType.DMA
    rows = 2 * planes
    scratch = [
        pltpu.VMEM((blocks, 2, CAP, half), BF16),
        *[pltpu.VMEM((n, planes, 2, CAP, part), BF16) for _ in range(6)],
        *[pltpu.VMEM((n - 1, tokens, part), BF16) for _ in range(3)],
        pltpu.VMEM((3, n - 1, 2 * top, tokens), BF16),
        pltpu.VMEM((3, n - 1, tokens, part), BF16),
        pltpu.VMEM((3, n - 1, tokens, part), BF16),
        pltpu.VMEM((n - 1, top, tokens), F32),
        pltpu.VMEM((n - 1, top, tokens), F32),
        pltpu.VMEM((3, n, rows, tokens), F32),
        pltpu.VMEM((3, n, rows, tokens), F32),
        pltpu.VMEM((2 * top, tokens), BF16),
        pltpu.VMEM((2, ff, half), BF16),
        pltpu.VMEM((2, ff, half), BF16),
        *[pltpu.VMEM((2, half, ff), BF16) for _ in range(4)],
        pltpu.VMEM((p.most * CAP, 2, ff), BF16),
        pltpu.VMEM((p.most * CAP, 2, ff), BF16),
        *[pltpu.VMEM((2, p.most * CAP, ff), F32) for _ in range(3)],
        *[pltpu.VMEM((2, p.most * CAP, 2 * ff + 128), BF16) for _ in range(2)],
        pltpu.VMEM((blocks, 1, 128), F32),
        pltpu.VMEM((n, planes, 1, 128), F32),
        dma((3,)), dma((3,)), dma((3,)), dma((3,)), dma((3, n - 1)),
        dma((3, nt)), dma((3, nt)), dma((2,)), dma((2,)), dma((2,)), dma((2,)),
        dma((3, 4)), dma((3, n)), dma((3,)), dma((3,)), dma((2,)),
        dma((1,)), dma((n,)), pltpu.SemaphoreType.REGULAR,
    ]
    grad_tokens, grad_combine = pl.pallas_call(
        functools.partial(kernel, p),
        out_shape=(
            jax.ShapeDtypeStruct((tokens, half), BF16),
            jax.ShapeDtypeStruct((top, tokens), BF16),
        ),
        in_specs=[vmem, vmem, vmem, hbm, hbm, hbm, hbm, hbm],
        out_specs=(vmem, vmem),
        scratch_shapes=scratch,
        compiler_params=pltpu.CompilerParams(
            collective_id=0, has_side_effects=True, vmem_limit_bytes=67043328
        ),
    )(expert_ids.T, combine.T, grad_out, saved_gate, saved_up, gate_weight, up_weight, down_weight)
    return grad_tokens, grad_combine.T


def solution(mesh, tiles=(27, 19, 18), step=256):
    n = round(mesh.shape["expert"] ** (1 / 3))

    def run(grad_out, combine, expert_ids, saved_gate, saved_up, gate_weight, up_weight, down_weight):
        plan = Plan(n, grad_out.shape[1], gate_weight.shape[2], expert_ids.shape[1], tiles, step)
        return on_device(
            plan, grad_out, combine, expert_ids, saved_gate, saved_up, gate_weight, up_weight, down_weight
        )

    in_specs = (
        P("expert", "etp"),
        P("expert", None),
        P("expert", None),
        P(None, "expert", "etp"),
        P(None, "expert", "etp"),
        P("expert", None, "etp"),
        P("expert", None, "etp"),
        P("expert", "etp", None),
    )
    out_specs = (P("expert", "etp"), P("expert", None))
    return jax.shard_map(run, mesh=mesh, in_specs=in_specs, out_specs=out_specs, check_vma=False)
```
